256 devices in a mesh: dp: 16 (over x, z_lo), owner: 16 (over z_hi, y, core).
Axes of the slice: x: 4, y: 4, z: 8 (z_hi: 2, z_lo: 4; z = z_hi * 4 + z_lo), core: 2. Of those that a mesh axis runs over, the one named last changes fastest.
Arguments:
- layer_input: bfloat16 [4096, 8192], P('dp', 'owner'), may hold values from -6 to 6
- output_grads: bfloat16 [4096, 10240], P('dp', 'owner'), may hold values from -6 to 6
- projection: bfloat16 [8192, 10240], P('owner', 'dp'), may hold values from -0.0625 to 0.0625
Outputs:
- grad_input: bfloat16 [4096, 8192], P('dp', 'owner')
- update_query: bfloat16 [8192, 8192], P('owner', 'dp')
- update_kv: bfloat16 [8192, 2048], P('owner', 'dp')
The draws below stay inside these ranges and needn't reach their ends.
All inputs are finite; a program needn't handle non-finite values.
Results may differ from the reference program's by a relative error of at most 0.023.
Values may be sent and summed in bfloat16 or wider, within the bound.
A program may use at most 128 MiB of HBM per device.

```python
import math
import jax
import jax.numpy as jnp
from jax import lax

D = 8192
BLOCK = 512
TOK_DEV = 256
QW = 8192
KVW = 2048
COLS = 10240
TOKENS = 4096
N_DP = 16


def strengthened(drawn, own_key, source, target, parts, factor):
    owner, partner = [(jnp.arange(drawn.shape[axis_at]) // (drawn.shape[axis_at] // parts)).reshape([-1 if axis == axis_at else 1 for axis in range(drawn.ndim)]) for axis_at in (source, target)]
    chosen = jax.random.permutation(own_key, parts)[partner]
    strong = (owner == chosen) | (owner == (partner + parts // 2) % parts)
    return jnp.where(strong, factor * drawn, drawn)


def steps_of(own_key, dims, cuts, low, largest):
    def one(axis_at, shards_of):
        heights = jax.random.uniform(jax.random.fold_in(jax.random.fold_in(own_key, 6), axis_at), (shards_of,), jnp.float32, low / len(cuts), largest / len(cuts))
        return jnp.repeat(jnp.exp(heights), dims[axis_at] // shards_of).reshape((-1,) + (1,) * (len(dims) - axis_at - 1))

    gain = one(*cuts[0])
    for cut in cuts[1:]:
        gain = gain * one(*cut)
    return gain


def gaussian(stream_key, dims, spread, reach, cuts=(), kind=jnp.bfloat16):
    array = jax.random.normal(stream_key, dims, jnp.float32) * spread
    if len(cuts) > 0:
        array = steps_of(stream_key, dims, cuts, -0.22, 0.18) * array
    return jnp.clip(array, min=-reach, max=reach).astype(kind)


def heavy_noise(stream_key, extent, spread, bound, cuts, heavy, kind=jnp.bfloat16):
    entries = spread * jax.random.normal(stream_key, extent, jnp.float32)
    if cuts:
        entries = entries * steps_of(stream_key, extent, cuts, -0.22, 0.18)
    return jnp.clip(strengthened(entries, jax.random.fold_in(stream_key, 3), *heavy), -bound, bound).astype(kind)


def setup_inputs(seed: int = 0) -> dict:
    keys = jax.random.split(jax.random.key(seed), 4)
    layer_input = gaussian(keys[0], (TOKENS, D), 1.0, 6.0, ((0, 16), (1, 16)))
    output_grads = heavy_noise(keys[1], (TOKENS, COLS), 1.0, 6.0, ((0, 16), (1, 16)), (0, 1, 16, 2.0))
    projection = gaussian(keys[2], (D, COLS), D ** -0.5, 0.0625, ((0, 16), (1, 16)))
    return {"layer_input": layer_input, "output_grads": output_grads, "projection": projection}


def left_stat(blocks):
    floats = blocks.astype(jnp.float32)
    return jnp.einsum('...ij,...kj->...ik', floats, floats, precision=lax.Precision.HIGHEST)

def right_stat(blocks):
    floats = blocks.astype(jnp.float32)
    return jnp.einsum('...ji,...jk->...ik', floats, floats, precision=lax.Precision.HIGHEST)

def inverse_root(statistic):
    width = statistic.shape[-1]
    scale = math.sqrt(width) * jnp.sqrt(lax.optimization_barrier(jnp.mean(statistic * statistic, axis=(-2, -1), keepdims=True)) + 1e-06)
    normed = statistic / scale
    identity = jnp.eye(width, dtype=jnp.float32)
    return scale ** (-0.25) * (5.0 * identity - normed) * 0.25

def precondition(blocks):
    width = blocks.shape[-1]
    root_left = inverse_root(left_stat(blocks))
    root_right = inverse_root(right_stat(blocks))
    half = jnp.einsum('...ij,...jk->...ik', blocks.astype(jnp.float32), root_right, precision=lax.Precision.HIGHEST)
    whole = jnp.einsum('...ij,...jk->...ik', root_left, half, precision=lax.Precision.HIGHEST)
    return (whole * math.sqrt(width)).astype(jnp.bfloat16)

def update_rows(rowset):
    columns = rowset.shape[1]
    blocks = rowset.reshape(BLOCK, columns // BLOCK, BLOCK).transpose(1, 0, 2)
    return precondition(blocks).transpose(1, 0, 2).reshape(BLOCK, columns)

def reference(layer_input, output_grads, projection):
    grad_input = jnp.dot(output_grads, projection.T, preferred_element_type=jnp.float32).astype(jnp.bfloat16)
    inputs_grouped = layer_input.reshape(N_DP, TOK_DEV, layer_input.shape[1])
    grads_grouped = output_grads.reshape(N_DP, TOK_DEV, output_grads.shape[1])

    def accumulate(running, pair):
        partial_value = jnp.dot(pair[0].T, pair[1], preferred_element_type=jnp.float32).astype(jnp.bfloat16)
        partial_value = lax.optimization_barrier(partial_value)
        return (running + partial_value.astype(jnp.float32), None)
    initial = jnp.zeros((layer_input.shape[1], output_grads.shape[1]), jnp.float32)
    summed, _ = lax.scan(accumulate, initial, (inputs_grouped, grads_grouped))
    gradient = summed.astype(jnp.bfloat16)
    rowsets = gradient.reshape(gradient.shape[0] // BLOCK, BLOCK, gradient.shape[1])
    update_query = lax.map(update_rows, rowsets[:, :, :QW]).reshape(gradient.shape[0], QW)
    update_kv = lax.map(update_rows, rowsets[:, :, QW:]).reshape(gradient.shape[0], KVW)
    return (grad_input, update_query, update_kv)
```

```python
import functools
import math

import jax
import jax.numpy as jnp
from jax import lax
from jax.experimental import pallas as pl
from jax.experimental.pallas import tpu as pltpu
from jax.sharding import PartitionSpec as P

BLOCK = 512
UNIT = 128
SLOTS = 20
VMEM_LIMIT = 60 * 1024 * 1024
BF16 = jnp.bfloat16
F32 = jnp.float32


class Place:
    def __init__(self):
        dp = lax.axis_index("dp")
        owner = lax.axis_index("owner")
        self.x = dp // 4
        self.z = dp % 4
        self.zh = owner // 8
        self.y = (owner // 2) % 4
        self.c = owner % 2
        self.dp = dp
        self.owner = owner

    def at(self, x=None, z=None, zh=None, y=None, c=None):
        x = self.x if x is None else x
        z = self.z if z is None else z
        zh = self.zh if zh is None else zh
        y = self.y if y is None else y
        c = self.c if c is None else c
        return (x * 4 + z, zh * 8 + y * 2 + c)


def unit_of(z, slot):
    group = slot // 5
    step = slot % 5
    kv = step // 4
    return (1 - kv) * (16 * group + 4 * z + step) + kv * (64 + 4 * group + z)


def slot_of(unit):
    kv = unit // 64
    z = (1 - kv) * ((unit // 4) % 4) + kv * (unit % 4)
    slot = (1 - kv) * (5 * (unit // 16) + unit % 4) + kv * (5 * ((unit - 64 * kv) // 4) + 4)
    return z, slot


def remote(src, dst, send, recv, device):
    return pltpu.make_async_remote_copy(
        src_ref=src,
        dst_ref=dst,
        send_sem=send,
        recv_sem=recv,
        device_id=device,
        device_id_type=pl.DeviceIdType.MESH,
    )


def cols(slot):
    return pl.ds(pl.multiple_of(slot * UNIT, UNIT), UNIT)


def greet(devices):
    barrier = pltpu.get_barrier_semaphore()
    for device in devices:
        pl.semaphore_signal(barrier, inc=1, device_id=device, device_id_type=pl.DeviceIdType.MESH)
    pl.semaphore_wait(barrier, len(devices))


def gather_kernel(x_ref, g_ref, p_ref, xg, gd, pg, gs1, gs, gr, ps1, ps, pr, xs, xr):
    me = Place()
    tokens = g_ref.shape[0]
    rows = p_ref.shape[0]
    half = rows // 2
    devices = []
    for step in range(1, 8):
        far = (me.zh * 4 + me.z + step) % 8
        devices.append(me.at(z=far % 4, zh=far // 4))
    yp, ym = (me.y + 1) % 4, (me.y + 3) % 4
    xp, xm = (me.x + 1) % 4, (me.x + 3) % 4
    devices += [me.at(y=yp), me.at(y=ym), me.at(c=1 - me.c), me.at(x=xp), me.at(x=xm)]
    greet(devices)

    def mine(z):
        return pl.ds(pl.multiple_of(z * tokens, tokens), tokens)

    for k in range(5):
        q, slot = slot_of(5 * me.owner + k)
        src = g_ref.at[:, k * UNIT : (k + 1) * UNIT]
        dst = gd.at[mine(me.z), cols(slot)]
        for zh in range(2):
            here = jnp.logical_and(q == me.z, me.zh == zh)

            @pl.when(here)
            def _():
                pltpu.make_async_copy(src, dst, gr.at[slot, me.z]).start()

            @pl.when(jnp.logical_not(here))
            def _():
                remote(src, dst, gs1.at[k, zh], gr.at[slot, me.z], me.at(z=q, zh=zh)).start()

    for k in range(5):
        q, slot = slot_of(5 * me.dp + k)
        src = p_ref.at[:, k * UNIT : (k + 1) * UNIT]
        dst = pg.at[:, cols(slot)]

        @pl.when(q == me.z)
        def _():
            pltpu.make_async_copy(src, dst, pr.at[slot, 0]).start()

        @pl.when(q != me.z)
        def _():
            remote(src, dst, ps1.at[k], pr.at[slot, 0], me.at(z=q)).start()

    def x_send(src, origin, side):
        to = me.z + 1 if side == 0 else me.z - 1
        return remote(src, xg.at[mine(origin)], xs.at[side, origin], xr.at[origin], me.at(z=to))

    own_x = pltpu.make_async_copy(x_ref, xg.at[mine(me.z)], xr.at[me.z])
    own_x.start()

    @pl.when(me.z < 3)
    def _():
        x_send(x_ref, me.z, 0).start()

    @pl.when(me.z > 0)
    def _():
        x_send(x_ref, me.z, 1).start()

    own_x.wait()

    def x_step(step):
        low = me.z - step
        high = me.z + step

        @pl.when(low >= 0)
        def _():
            slot = jnp.maximum(low, 0)
            block = xg.at[mine(slot)]
            pltpu.make_async_copy(x_ref, block, xr.at[slot]).wait()

            @pl.when(me.z < 3)
            def _():
                x_send(block, slot, 0).start()

        @pl.when(high <= 3)
        def _():
            slot = jnp.minimum(high, 3)
            block = xg.at[mine(slot)]
            pltpu.make_async_copy(x_ref, block, xr.at[slot]).wait()

            @pl.when(me.z > 0)
            def _():
                x_send(block, slot, 1).start()

    def g_parts(slot):
        unit = unit_of(me.z, slot)
        dy = (me.y - (unit // 10) % 4 + 4) % 4
        ring = (unit // 5) % 2 == me.c
        whole = gd.at[:, cols(slot)]
        upper = gd.at[0 : 2 * tokens, cols(slot)]
        lower = gd.at[2 * tokens : 4 * tokens, cols(slot)]
        return dy, ring, whole, upper, lower

    def g_send(part, slot, way, index=0):
        device = (me.at(y=yp), me.at(y=ym), me.at(c=1 - me.c))[way]
        return remote(part, part, gs.at[slot, way], gr.at[slot, index], device)

    def g_wait(part, slot, index):
        pltpu.make_async_copy(part, part, gr.at[slot, index]).wait()

    def p_parts(slot):
        unit = unit_of(me.z, slot)
        dx = (me.x - unit // 20 + 4) % 4
        whole = pg.at[:, cols(slot)]
        upper = pg.at[0:half, cols(slot)]
        lower = pg.at[half:rows, cols(slot)]
        return dx, whole, upper, lower

    def p_send(part, slot, way, index=0):
        device = (me.at(x=xp), me.at(x=xm))[way]
        return remote(part, part, ps.at[slot, way], pr.at[slot, index], device)

    def p_wait(part, slot, index):
        pltpu.make_async_copy(part, part, pr.at[slot, index]).wait()

    @pl.loop(0, SLOTS)
    def _(slot):
        dy, ring, whole, upper, lower = g_parts(slot)

        @pl.when(jnp.logical_and(ring, dy == 0))
        def _():
            for t in range(4):
                g_wait(gd.at[t * tokens : (t + 1) * tokens, cols(slot)], slot, t)
            g_send(whole, slot, 0).start()
            g_send(whole, slot, 1).start()
            g_send(whole, slot, 2).start()

    @pl.loop(0, SLOTS)
    def _(slot):
        dx, whole, upper, lower = p_parts(slot)

        @pl.when(dx == 0)
        def _():
            p_wait(whole, slot, 0)
            p_send(whole, slot, 0).start()
            p_send(whole, slot, 1).start()

    x_step(1)

    @pl.loop(0, SLOTS)
    def _(slot):
        dy, ring, whole, upper, lower = g_parts(slot)

        @pl.when(jnp.logical_and(ring, dy == 1))
        def _():
            g_wait(whole, slot, 0)
            g_send(upper, slot, 0).start()
            g_send(whole, slot, 2).start()

        @pl.when(jnp.logical_and(ring, dy == 3))
        def _():
            g_wait(whole, slot, 0)
            g_send(lower, slot, 1, 1).start()
            g_send(whole, slot, 2).start()

    x_step(2)

    @pl.loop(0, SLOTS)
    def _(slot):
        dx, whole, upper, lower = p_parts(slot)

        @pl.when(dx == 1)
        def _():
            p_wait(whole, slot, 0)
            p_send(upper, slot, 0).start()

        @pl.when(dx == 3)
        def _():
            p_wait(whole, slot, 0)
            p_send(lower, slot, 1, 1).start()

    @pl.loop(0, SLOTS)
    def _(slot):
        dy, ring, whole, upper, lower = g_parts(slot)

        @pl.when(jnp.logical_and(ring, dy == 2))
        def _():
            g_wait(upper, slot, 0)
            g_wait(lower, slot, 1)
            g_send(whole, slot, 2).start()

    x_step(3)

    @pl.loop(0, SLOTS)
    def _(slot):
        dx, whole, upper, lower = p_parts(slot)

        @pl.when(dx == 2)
        def _():
            p_wait(upper, slot, 0)
            p_wait(lower, slot, 1)

    @pl.loop(0, SLOTS)
    def _(slot):
        dy, ring, whole, upper, lower = g_parts(slot)

        @pl.when(jnp.logical_not(ring))
        def _():
            g_wait(whole, slot, 0)

    for k in range(5):
        q, slot = slot_of(5 * me.owner + k)
        src = g_ref.at[:, k * UNIT : (k + 1) * UNIT]
        for zh in range(2):
            @pl.when(jnp.logical_not(jnp.logical_and(q == me.z, me.zh == zh)))
            def _():
                pltpu.make_async_copy(src, src, gs1.at[k, zh]).wait()

        q, slot = slot_of(5 * me.dp + k)
        psrc = p_ref.at[:, k * UNIT : (k + 1) * UNIT]

        @pl.when(q != me.z)
        def _():
            pltpu.make_async_copy(psrc, psrc, ps1.at[k]).wait()

    for origin in range(4):
        block = xg.at[origin * tokens : (origin + 1) * tokens]

        @pl.when(jnp.logical_and(origin <= me.z, me.z < 3))
        def _():
            pltpu.make_async_copy(block, block, xs.at[0, origin]).wait()

        @pl.when(jnp.logical_and(origin >= me.z, me.z > 0))
        def _():
            pltpu.make_async_copy(block, block, xs.at[1, origin]).wait()

    @pl.loop(0, SLOTS)
    def _(slot):
        dy, ring, whole, upper, lower = g_parts(slot)

        @pl.when(ring)
        def _():
            pltpu.make_async_copy(whole, whole, gs.at[slot, 2]).wait()

        @pl.when(jnp.logical_and(ring, dy == 0))
        def _():
            pltpu.make_async_copy(whole, whole, gs.at[slot, 0]).wait()
            pltpu.make_async_copy(whole, whole, gs.at[slot, 1]).wait()

        @pl.when(jnp.logical_and(ring, dy == 1))
        def _():
            pltpu.make_async_copy(upper, upper, gs.at[slot, 0]).wait()

        @pl.when(jnp.logical_and(ring, dy == 3))
        def _():
            pltpu.make_async_copy(lower, lower, gs.at[slot, 1]).wait()

        dx, whole, upper, lower = p_parts(slot)

        @pl.when(dx == 0)
        def _():
            pltpu.make_async_copy(whole, whole, ps.at[slot, 0]).wait()
            pltpu.make_async_copy(whole, whole, ps.at[slot, 1]).wait()

        @pl.when(dx == 1)
        def _():
            pltpu.make_async_copy(upper, upper, ps.at[slot, 0]).wait()

        @pl.when(dx == 3)
        def _():
            pltpu.make_async_copy(lower, lower, ps.at[slot, 1]).wait()


def exchange_kernel(w_ref, c_ref, wr, cr, fw, ws, wv, fs, fv, cs, cv, own):
    me = Place()
    width = wr.shape[2]
    half = wr.shape[1] // 2
    tokens = cr.shape[1]
    xp, xm, xo = (me.x + 1) % 4, (me.x + 3) % 4, (me.x + 2) % 4
    devices = [me.at(x=xp), me.at(x=xm)]
    for step in range(1, 4):
        devices.append(me.at(z=(me.z + step) % 4))
    greet(devices)

    def chunk(x):
        return pl.ds(pl.multiple_of(x * width, UNIT), width)

    first = [
        remote(w_ref.at[0:half, chunk(xo)], fw.at[0], fs.at[0], fv.at[0], me.at(x=xp)),
        remote(w_ref.at[half : 2 * half, chunk(xo)], fw.at[1], fs.at[1], fv.at[1], me.at(x=xm)),
    ]
    for copy in first:
        copy.start()
    direct = [
        remote(w_ref.at[:, chunk(xp)], wr.at[1], ws.at[0], wv.at[0], me.at(x=xp)),
        remote(w_ref.at[:, chunk(xm)], wr.at[3], ws.at[1], wv.at[1], me.at(x=xm)),
    ]
    for copy in direct:
        copy.start()
    for step in range(1, 4):
        to = (me.z + step) % 4
        copy = remote(
            c_ref.at[pl.ds(pl.multiple_of(to * tokens, tokens), tokens)],
            cr.at[step],
            cs.at[step],
            cv.at[step],
            me.at(z=to),
        )
        copy.start()
        direct.append(copy)
    mine = [
        pltpu.make_async_copy(w_ref.at[:, chunk(me.x)], wr.at[0], own.at[0]),
        pltpu.make_async_copy(
            c_ref.at[pl.ds(pl.multiple_of(me.z * tokens, tokens), tokens)], cr.at[0], own.at[1]
        ),
    ]
    for copy in mine:
        copy.start()
    first[0].wait_recv()
    second = [remote(fw.at[0], wr.at[2, 0:half], ws.at[2], wv.at[2], me.at(x=xp))]
    second[0].start()
    first[1].wait_recv()
    second.append(
        remote(fw.at[1], wr.at[2, half : 2 * half], ws.at[3], wv.at[3], me.at(x=xm))
    )
    second[1].start()
    for copy in first:
        copy.wait_send()
    for copy in mine + direct + second:
        copy.wait()


def spread_kernel(w_ref, out, send, recv, own):
    me = Place()
    devices = [me.at(z=(me.z + step) % 4) for step in range(1, 4)]
    greet(devices)
    mine = pltpu.make_async_copy(w_ref, out.at[0], own)
    mine.start()
    copies = [
        remote(w_ref, out.at[step], send.at[step], recv.at[step], devices[step - 1])
        for step in range(1, 4)
    ]
    for copy in copies:
        copy.start()
    mine.wait()
    for copy in copies:
        copy.wait()


def call(kernel, name, ident, outs, scratch, *operands):
    vmem = pl.BlockSpec(memory_space=pltpu.VMEM)
    return pl.pallas_call(
        kernel,
        name=name,
        out_shape=outs,
        in_specs=[pl.BlockSpec(memory_space=pl.ANY)] * len(operands),
        out_specs=jax.tree.map(lambda _: vmem, outs),
        scratch_shapes=scratch,
        compiler_params=pltpu.CompilerParams(
            collective_id=ident, has_side_effects=True, vmem_limit_bytes=VMEM_LIMIT
        ),
    )(*operands)


def dma(*shape):
    return pltpu.SemaphoreType.DMA(shape) if shape else pltpu.SemaphoreType.DMA


def split(value):
    high = value.astype(BF16)
    return high, (value - high.astype(F32)).astype(BF16)


def mm(a, b):
    return lax.dot_general(a, b, (((1,), (0,)), ((), ())), preferred_element_type=F32)


def update_of(left, target):
    width = left.shape[0]
    scale = math.sqrt(width) * jnp.sqrt(jnp.mean(left * left) + 1e-06)
    lh, ll = split(left / scale)
    once = mm(lh, target) + mm(ll, target)
    oh, ol = split(once)
    twice = mm(lh, oh) + mm(ll, oh) + mm(lh, ol)
    factor = math.sqrt(width) / 16.0 * lax.rsqrt(scale)
    return (factor * (25.0 * target.astype(F32) - 10.0 * once + twice)).astype(BF16)


def left_of(block):
    return lax.dot_general(block, block, (((1,), (1,)), ((), ())), preferred_element_type=F32)


def precondition_kernel(w_ref, kv_ref, uq, ukv):
    width = w_ref.shape[0]
    square = w_ref[:, 0:width]
    uq[...] = update_of(left_of(square), square)
    left = left_of(kv_ref[0])
    for part in range(1, 4):
        left += left_of(kv_ref[part])
    ukv[...] = update_of(left, kv_ref[0])


def body(layer_input, output_grads, projection):
    tokens, rows = layer_input.shape
    chunk = output_grads.shape[1]
    shape = jax.ShapeDtypeStruct
    xg, gd, pg = call(
        gather_kernel,
        "gather",
        0,
        (
            shape((4 * tokens, rows), BF16),
            shape((4 * tokens, SLOTS * UNIT), BF16),
            shape((rows, SLOTS * UNIT), BF16),
        ),
        [
            dma(5, 2),
            dma(SLOTS, 3),
            dma(SLOTS, 4),
            dma(5),
            dma(SLOTS, 2),
            dma(SLOTS, 2),
            dma(2, 4),
            dma(4),
        ],
        layer_input,
        output_grads,
        projection,
    )
    w_part = jnp.einsum("tr,tc->rc", xg, gd, preferred_element_type=F32).astype(BF16)
    c_part = jnp.einsum("tc,rc->tr", gd, pg, preferred_element_type=F32).astype(BF16)
    wr, cr = call(
        exchange_kernel,
        "exchange",
        1,
        (shape((4, rows, chunk), BF16), shape((4, tokens, rows), BF16)),
        [pltpu.VMEM((2, rows // 2, chunk), BF16), dma(4), dma(4), dma(2), dma(2), dma(4), dma(4), dma(2)],
        w_part,
        c_part,
    )
    grads = jnp.sum(wr.astype(F32), axis=0).astype(BF16)
    grad_input = jnp.sum(cr.astype(F32), axis=0).astype(BF16)
    kv = call(
        spread_kernel,
        "spread",
        2,
        shape((4, rows, UNIT), BF16),
        [dma(4), dma(4), dma()],
        grads[:, BLOCK:],
    )
    vmem = pl.BlockSpec(memory_space=pltpu.VMEM)
    update_query, update_kv = pl.pallas_call(
        precondition_kernel,
        name="precondition",
        out_shape=(shape((rows, BLOCK), BF16), shape((rows, UNIT), BF16)),
        in_specs=[vmem, vmem],
        out_specs=(vmem, vmem),
        compiler_params=pltpu.CompilerParams(vmem_limit_bytes=VMEM_LIMIT),
    )(grads, kv)
    return (grad_input, update_query, update_kv)


def solution(mesh):
    placed = (P("dp", "owner"), P("dp", "owner"), P("owner", "dp"))
    return jax.shard_map(
        body,
        mesh=mesh,
        in_specs=placed,
        out_specs=(P("dp", "owner"), P("owner", "dp"), P("owner", "dp")),
        check_vma=False,
    )
```

```python
import math

import jax
import jax.numpy as jnp
from jax import lax
from jax.experimental import pallas as pl
from jax.experimental.pallas import tpu as pltpu
from jax.sharding import PartitionSpec as P

BLOCK = 512
UNIT = 128
SLOTS = 20
VMEM_LIMIT = 60 * 1024 * 1024
BF16 = jnp.bfloat16
F32 = jnp.float32


class Place:
    def __init__(self):
        dp = lax.axis_index("dp")
        owner = lax.axis_index("owner")
        self.x = dp // 4
        self.z = dp % 4
        self.zh = owner // 8
        self.y = (owner // 2) % 4
        self.c = owner % 2
        self.dp = dp
        self.owner = owner

    def at(self, x=None, z=None, zh=None, y=None, c=None):
        x = self.x if x is None else x
        z = self.z if z is None else z
        zh = self.zh if zh is None else zh
        y = self.y if y is None else y
        c = self.c if c is None else c
        return (x * 4 + z, zh * 8 + y * 2 + c)


def unit_of(z, slot):
    group = slot // 5
    step = slot % 5
    kv = step // 4
    return (1 - kv) * (16 * group + 4 * z + step) + kv * (64 + 4 * group + z)


def slot_of(unit):
    kv = unit // 64
    z = (1 - kv) * ((unit // 4) % 4) + kv * (unit % 4)
    slot = (1 - kv) * (5 * (unit // 16) + unit % 4) + kv * (5 * ((unit - 64 * kv) // 4) + 4)
    return z, slot


def remote(src, dst, send, recv, device):
    return pltpu.make_async_remote_copy(
        src_ref=src,
        dst_ref=dst,
        send_sem=send,
        recv_sem=recv,
        device_id=device,
        device_id_type=pl.DeviceIdType.MESH,
    )


def cols(slot):
    return pl.ds(pl.multiple_of(slot * UNIT, UNIT), UNIT)


def greet(devices):
    barrier = pltpu.get_barrier_semaphore()
    for device in devices:
        pl.semaphore_signal(barrier, inc=1, device_id=device, device_id_type=pl.DeviceIdType.MESH)
    pl.semaphore_wait(barrier, len(devices))


def fused_kernel(
    x_ref, g_ref, p_ref, out_c, out_q, out_kv,
    xg, xt, gd, pg, kp, qp, kf, qf, kl, kr, ql, qr, kv, cp, ca, cb,
    gs1, gs, gr, ps1, ps, pr, xs, xr,
    fks, fkr, fqs, fqr, ks, kvr, qs, qvr, ss, sr, cs, crv,
):
    me = Place()
    tokens = g_ref.shape[0]
    rows = p_ref.shape[0]
    half = rows // 2
    yp, ym, yo = (me.y + 1) % 4, (me.y + 3) % 4, (me.y + 2) % 4
    xp, xm, xo = (me.x + 1) % 4, (me.x + 3) % 4, (me.x + 2) % 4
    devices = []
    for step in range(1, 8):
        far = (me.zh * 4 + me.z + step) % 8
        devices.append(me.at(z=far % 4, zh=far // 4))
    devices += [me.at(y=yp), me.at(y=ym), me.at(c=1 - me.c), me.at(x=xp), me.at(x=xm)]
    greet(devices)

    def mine(z):
        return pl.ds(pl.multiple_of(z * tokens, tokens), tokens)

    def wait_for(part, sem):
        pltpu.make_async_copy(part, part, sem).wait()

    for k in range(5):
        q, slot = slot_of(5 * me.owner + k)
        src = g_ref.at[:, k * UNIT : (k + 1) * UNIT]
        dst = gd.at[mine(me.z), cols(slot)]
        for zh in range(2):
            here = jnp.logical_and(q == me.z, me.zh == zh)

            @pl.when(here)
            def _():
                pltpu.make_async_copy(src, dst, gr.at[slot, me.z]).start()

            @pl.when(jnp.logical_not(here))
            def _():
                remote(src, dst, gs1.at[k, zh], gr.at[slot, me.z], me.at(z=q, zh=zh)).start()

    for k in range(5):
        q, slot = slot_of(5 * me.dp + k)
        src = p_ref.at[:, k * UNIT : (k + 1) * UNIT]
        dst = pg.at[:, cols(slot)]

        @pl.when(q == me.z)
        def _():
            pltpu.make_async_copy(src, dst, pr.at[slot, 0]).start()

        @pl.when(q != me.z)
        def _():
            remote(src, dst, ps1.at[k], pr.at[slot, 0], me.at(z=q)).start()

    def x_send(src, origin, side):
        to = me.z + 1 if side == 0 else me.z - 1
        return remote(src, xg.at[mine(origin)], xs.at[side, origin], xr.at[origin], me.at(z=to))

    own_x = pltpu.make_async_copy(x_ref, xg.at[mine(me.z)], xr.at[me.z])
    own_x.start()

    @pl.when(me.z < 3)
    def _():
        x_send(x_ref, me.z, 0).start()

    @pl.when(me.z > 0)
    def _():
        x_send(x_ref, me.z, 1).start()

    own_x.wait()

    def x_step(step):
        low = me.z - step
        high = me.z + step

        @pl.when(low >= 0)
        def _():
            slot = jnp.maximum(low, 0)
            block = xg.at[mine(slot)]
            wait_for(block, xr.at[slot])

            @pl.when(me.z < 3)
            def _():
                x_send(block, slot, 0).start()

        @pl.when(high <= 3)
        def _():
            slot = jnp.minimum(high, 3)
            block = xg.at[mine(slot)]
            wait_for(block, xr.at[slot])

            @pl.when(me.z > 0)
            def _():
                x_send(block, slot, 1).start()

    def g_unit(y, c, zh, k):
        q, slot = slot_of(5 * (8 * zh + 2 * y + c) + k)
        whole = gd.at[:, cols(slot)]
        upper = gd.at[0 : 2 * tokens, cols(slot)]
        lower = gd.at[2 * tokens : 4 * tokens, cols(slot)]
        return q == me.z, slot, whole, upper, lower

    def g_send(part, slot, way, index=0):
        device = (me.at(y=yp), me.at(y=ym), me.at(c=1 - me.c))[way]
        return remote(part, part, gs.at[slot, way], gr.at[slot, index], device)

    def p_unit(x, z, k):
        q, slot = slot_of(5 * (4 * x + z) + k)
        whole = pg.at[:, cols(slot)]
        upper = pg.at[0:half, cols(slot)]
        lower = pg.at[half:rows, cols(slot)]
        return q == me.z, slot, whole, upper, lower

    def p_send(part, slot, way, index=0):
        device = (me.at(x=xp), me.at(x=xm))[way]
        return remote(part, part, ps.at[slot, way], pr.at[slot, index], device)

    def g_origin(k, waiting):
        for zh in range(2):
            ok, slot, whole, upper, lower = g_unit(me.y, me.c, zh, k)

            @pl.when(ok)
            def _():
                if waiting:
                    for way in range(3):
                        wait_for(whole, gs.at[slot, way])
                else:
                    for t in range(4):
                        wait_for(gd.at[t * tokens : (t + 1) * tokens, cols(slot)], gr.at[slot, t])
                    for way in range(3):
                        g_send(whole, slot, way).start()

    def g_next(k, waiting):
        for zh in range(2):
            for side, y in ((0, ym), (1, yp)):
                ok, slot, whole, upper, lower = g_unit(y, me.c, zh, k)
                part = upper if side == 0 else lower

                @pl.when(ok)
                def _():
                    if waiting:
                        wait_for(part, gs.at[slot, side])
                        wait_for(whole, gs.at[slot, 2])
                    else:
                        wait_for(whole, gr.at[slot, 0])
                        g_send(part, slot, side, side).start()
                        g_send(whole, slot, 2).start()

    def g_last(k, waiting):
        for zh in range(2):
            ok, slot, whole, upper, lower = g_unit(yo, me.c, zh, k)

            @pl.when(ok)
            def _():
                if waiting:
                    wait_for(whole, gs.at[slot, 2])
                else:
                    wait_for(upper, gr.at[slot, 0])
                    wait_for(lower, gr.at[slot, 1])
                    g_send(whole, slot, 2).start()

    def g_sibling(k):
        for zh in range(2):
            for y in range(4):
                ok, slot, whole, upper, lower = g_unit(y, 1 - me.c, zh, k)

                @pl.when(ok)
                def _():
                    wait_for(whole, gr.at[slot, 0])

    def p_origin(k, waiting):
        for z in range(4):
            ok, slot, whole, upper, lower = p_unit(me.x, z, k)

            @pl.when(ok)
            def _():
                if waiting:
                    for way in range(2):
                        wait_for(whole, ps.at[slot, way])
                else:
                    wait_for(whole, pr.at[slot, 0])
                    for way in range(2):
                        p_send(whole, slot, way).start()

    def p_next(k, waiting):
        for z in range(4):
            for side, x in ((0, xm), (1, xp)):
                ok, slot, whole, upper, lower = p_unit(x, z, k)
                part = upper if side == 0 else lower

                @pl.when(ok)
                def _():
                    if waiting:
                        wait_for(part, ps.at[slot, side])
                    else:
                        wait_for(whole, pr.at[slot, 0])
                        p_send(part, slot, side, side).start()

    def p_last(k):
        for z in range(4):
            ok, slot, whole, upper, lower = p_unit(xo, z, k)

            @pl.when(ok)
            def _():
                wait_for(upper, pr.at[slot, 0])
                wait_for(lower, pr.at[slot, 1])

    @pl.loop(0, 5)
    def _(k):
        g_origin(k, False)
        p_origin(k, False)

    x_step(1)

    @pl.loop(0, 5)
    def _(k):
        g_next(k, False)
        p_next(k, False)

    x_step(2)

    @pl.loop(0, 5)
    def _(k):
        g_last(k, False)

    x_step(3)

    @pl.loop(0, 4)
    def _(t):
        xt[:, mine(t)] = xg[mine(t), :].T

    @pl.loop(0, 5)
    def _(k):
        g_sibling(k)

    def w_dot(x, first, count):
        at = pl.ds(pl.multiple_of((5 * x + first) * UNIT, UNIT), count * UNIT)
        return mm(xt[...], gd[:, at]).astype(BF16)

    kp[0] = w_dot(xo, 4, 1)
    kp[1] = w_dot(xp, 4, 1)
    kp[2] = w_dot(xm, 4, 1)
    plus, minus = me.at(x=xp), me.at(x=xm)
    raw_k = [
        remote(kp.at[0, 0:half], kf.at[0], fks.at[0], fkr.at[0], plus),
        remote(kp.at[0, half:rows], kf.at[1], fks.at[1], fkr.at[1], minus),
    ]
    own_k = [
        remote(kp.at[1, half:rows], kl.at[half:rows], ks.at[0], kvr.at[0], plus),
        remote(kp.at[2, 0:half], kr.at[0:half], ks.at[1], kvr.at[1], minus),
    ]
    for copy in raw_k + own_k:
        copy.start()
    qp[0] = w_dot(xo, 0, 4)
    raw_q = [
        remote(qp.at[0, 0:half], qf.at[0], fqs.at[0], fqr.at[0], plus),
        remote(qp.at[0, half:rows], qf.at[1], fqs.at[1], fqr.at[1], minus),
    ]
    for copy in raw_q:
        copy.start()
    qp[1] = w_dot(xp, 0, 4)
    qp[2] = w_dot(xm, 0, 4)
    own_q = [
        remote(qp.at[1, half:rows], ql.at[half:rows], qs.at[0], qvr.at[0], plus),
        remote(qp.at[2, 0:half], qr.at[0:half], qs.at[1], qvr.at[1], minus),
    ]
    for copy in own_q:
        copy.start()

    def add(a, b):
        return (a.astype(F32) + b.astype(F32)).astype(BF16)

    for copy in raw_k:
        copy.wait_recv()
    kf[0] = add(kf[0], kp[1, 0:half])
    kf[1] = add(kf[1], kp[2, half:rows])
    sum_k = [
        remote(kf.at[0], kl.at[0:half], ks.at[2], kvr.at[2], plus),
        remote(kf.at[1], kr.at[half:rows], ks.at[3], kvr.at[3], minus),
    ]
    for copy in sum_k:
        copy.start()

    @pl.loop(0, 5)
    def _(k):
        p_last(k)

    def c_dot(d):
        block = gd[d * tokens : (d + 1) * tokens, :]
        cp[d] = lax.dot_general(
            block, pg[...], (((1,), (1,)), ((), ())), preferred_element_type=F32
        ).astype(BF16)

    def c_copy(d, side):
        buffer = ca if side == 0 else cb
        to = jnp.minimum(me.z + 1, 3) if side == 0 else jnp.maximum(me.z - 1, 0)
        return remote(cp.at[d], buffer.at[d], cs.at[d], crv.at[side, d], me.at(z=to))

    def c_step(step):
        d = 3 - step

        @pl.when(me.z < d)
        def _():
            @pl.when(me.z > 0)
            def _():
                wait_for(ca.at[d], crv.at[0, d])
                cp[d] = add(cp[d], ca[d])

            c_copy(d, 0).start()

        e = step

        @pl.when(me.z > e)
        def _():
            @pl.when(me.z < 3)
            def _():
                wait_for(cb.at[e], crv.at[1, e])
                cp[e] = add(cp[e], cb[e])

            c_copy(e, 1).start()

    c_dot(3)
    c_dot(0)
    c_step(0)

    for copy in raw_q:
        copy.wait_recv()
    qf[0] = add(qf[0], qp[1, 0:half])
    qf[1] = add(qf[1], qp[2, half:rows])
    sum_q = [
        remote(qf.at[0], ql.at[0:half], qs.at[2], qvr.at[2], plus),
        remote(qf.at[1], qr.at[half:rows], qs.at[3], qvr.at[3], minus),
    ]
    for copy in sum_q:
        copy.start()

    c_dot(2)
    c_dot(1)
    c_step(1)

    kw = mm(xt[...], gd[:, pl.ds(pl.multiple_of((5 * me.x + 4) * UNIT, UNIT), UNIT)])
    for copy in own_k + sum_k:
        copy.wait_recv()
    kv[me.z] = (kw + kl[...].astype(F32) + kr[...].astype(F32)).astype(BF16)

    def kv_send(origin, side):
        to = me.z + 1 if side == 0 else me.z - 1
        return remote(kv.at[origin], kv.at[origin], ss.at[side, origin], sr.at[origin], me.at(z=to))

    @pl.when(me.z < 3)
    def _():
        kv_send(me.z, 0).start()

    @pl.when(me.z > 0)
    def _():
        kv_send(me.z, 1).start()

    c_step(2)
    qw = mm(xt[...], gd[:, pl.ds(pl.multiple_of(5 * me.x * UNIT, UNIT), 4 * UNIT)])

    for step in range(1, 4):
        low = me.z - step
        high = me.z + step

        @pl.when(low >= 0)
        def _():
            slot = jnp.maximum(low, 0)
            wait_for(kv.at[slot], sr.at[slot])

            @pl.when(me.z < 3)
            def _():
                kv_send(slot, 0).start()

        @pl.when(high <= 3)
        def _():
            slot = jnp.minimum(high, 3)
            wait_for(kv.at[slot], sr.at[slot])

            @pl.when(me.z > 0)
            def _():
                kv_send(slot, 1).start()

    gram = left_of(kv[0])
    for part in range(1, 4):
        gram += left_of(kv[part])
    out_kv[...] = update_of(gram, kv[me.z])

    for copy in own_q + sum_q:
        copy.wait_recv()
    square = (qw + ql[...].astype(F32) + qr[...].astype(F32)).astype(BF16)
    out_q[...] = update_of(left_of(square), square)

    for d in range(4):
        @pl.when(me.z == d)
        def _():
            total = cp[d].astype(F32)
            if d > 0:
                wait_for(ca.at[d], crv.at[0, d])
                total += ca[d].astype(F32)
            if d < 3:
                wait_for(cb.at[d], crv.at[1, d])
                total += cb[d].astype(F32)
            out_c[...] = total.astype(BF16)

    for k in range(5):
        q, slot = slot_of(5 * me.owner + k)
        src = g_ref.at[:, k * UNIT : (k + 1) * UNIT]
        for zh in range(2):
            @pl.when(jnp.logical_not(jnp.logical_and(q == me.z, me.zh == zh)))
            def _():
                wait_for(src, gs1.at[k, zh])

        q, slot = slot_of(5 * me.dp + k)
        psrc = p_ref.at[:, k * UNIT : (k + 1) * UNIT]

        @pl.when(q != me.z)
        def _():
            wait_for(psrc, ps1.at[k])

    @pl.loop(0, 5)
    def _(k):
        g_origin(k, True)
        g_next(k, True)
        g_last(k, True)
        p_origin(k, True)
        p_next(k, True)

    for origin in range(4):
        block = xg.at[origin * tokens : (origin + 1) * tokens]

        @pl.when(jnp.logical_and(origin <= me.z, me.z < 3))
        def _():
            wait_for(block, xs.at[0, origin])
            wait_for(kv.at[origin], ss.at[0, origin])

        @pl.when(jnp.logical_and(origin >= me.z, me.z > 0))
        def _():
            wait_for(block, xs.at[1, origin])
            wait_for(kv.at[origin], ss.at[1, origin])

        @pl.when(me.z != origin)
        def _():
            wait_for(cp.at[origin], cs.at[origin])

    for copy in raw_k + own_k + sum_k + raw_q + own_q + sum_q:
        copy.wait_send()


def dma(*shape):
    return pltpu.SemaphoreType.DMA(shape)


def split(value):
    high = value.astype(BF16)
    return high, (value - high.astype(F32)).astype(BF16)


def mm(a, b):
    return lax.dot_general(a, b, (((1,), (0,)), ((), ())), preferred_element_type=F32)


def update_of(left, target):
    width = left.shape[0]
    scale = math.sqrt(width) * jnp.sqrt(jnp.mean(left * left) + 1e-06)
    lh, ll = split(left * (1.0 / scale))
    once = mm(lh, target) + mm(ll, target)
    oh, ol = split(once)
    twice = mm(lh, oh) + mm(ll, oh) + mm(lh, ol)
    factor = math.sqrt(width) / 16.0 * lax.rsqrt(scale)
    return (factor * (25.0 * target.astype(F32) - 10.0 * once + twice)).astype(BF16)


def left_of(block):
    return lax.dot_general(block, block, (((1,), (1,)), ((), ())), preferred_element_type=F32)


def body(layer_input, output_grads, projection):
    tokens, rows = layer_input.shape
    half = rows // 2
    shape = jax.ShapeDtypeStruct
    vmem = pl.BlockSpec(memory_space=pltpu.VMEM)

    def space(*dims):
        return pltpu.VMEM(dims, BF16)

    return pl.pallas_call(
        fused_kernel,
        name="fused",
        out_shape=(
            shape((tokens, rows), BF16),
            shape((rows, BLOCK), BF16),
            shape((rows, UNIT), BF16),
        ),
        in_specs=[pl.BlockSpec(memory_space=pl.ANY)] * 3,
        out_specs=(vmem, vmem, vmem),
        scratch_shapes=[
            space(4 * tokens, rows),
            space(rows, 4 * tokens),
            space(4 * tokens, SLOTS * UNIT),
            space(rows, SLOTS * UNIT),
            space(3, rows, UNIT),
            space(3, rows, BLOCK),
            space(2, half, UNIT),
            space(2, half, BLOCK),
            space(rows, UNIT),
            space(rows, UNIT),
            space(rows, BLOCK),
            space(rows, BLOCK),
            space(4, rows, UNIT),
            space(4, tokens, rows),
            space(4, tokens, rows),
            space(4, tokens, rows),
            dma(5, 2),
            dma(SLOTS, 3),
            dma(SLOTS, 4),
            dma(5),
            dma(SLOTS, 2),
            dma(SLOTS, 2),
            dma(2, 4),
            dma(4),
            dma(2),
            dma(2),
            dma(2),
            dma(2),
            dma(4),
            dma(4),
            dma(4),
            dma(4),
            dma(2, 4),
            dma(4),
            dma(4),
            dma(2, 4),
        ],
        compiler_params=pltpu.CompilerParams(
            collective_id=0, has_side_effects=True, vmem_limit_bytes=VMEM_LIMIT
        ),
    )(layer_input, output_grads, projection)


def solution(mesh):
    placed = (P("dp", "owner"), P("dp", "owner"), P("owner", "dp"))
    return jax.shard_map(
        body,
        mesh=mesh,
        in_specs=placed,
        out_specs=(P("dp", "owner"), P("owner", "dp"), P("owner", "dp")),
        check_vma=False,
    )
```

```python
import math

import jax
import jax.numpy as jnp
from jax import lax
from jax.experimental import pallas as pl
from jax.experimental.pallas import tpu as pltpu
from jax.sharding import PartitionSpec as P

BLOCK = 512
UNIT = 128
SLOTS = 20
VMEM_LIMIT = 60 * 1024 * 1024
BF16 = jnp.bfloat16
F32 = jnp.float32


class Place:
    def __init__(self):
        dp = lax.axis_index("dp")
        owner = lax.axis_index("owner")
        self.x = dp >> 2
        self.z = dp & 3
        self.zh = owner >> 3
        self.y = (owner >> 1) & 3
        self.c = owner & 1
        self.dp = dp
        self.owner = owner

    def at(self, x=None, z=None, zh=None, y=None, c=None):
        x = self.x if x is None else x
        z = self.z if z is None else z
        zh = self.zh if zh is None else zh
        y = self.y if y is None else y
        c = self.c if c is None else c
        return (x * 4 + z, zh * 8 + y * 2 + c)


def unit_of(z, slot):
    group = slot // 5
    step = slot % 5
    kv = step // 4
    return (1 - kv) * (16 * group + 4 * z + step) + kv * (64 + 4 * group + z)


def slot_of(unit):
    kv = unit >> 6
    group = unit >> 2
    low = unit - (group << 2)
    rest = group & 3
    z = rest + kv * (low - rest)
    slot = 5 * (unit >> 4) + low + kv * (5 * (group - 16) + 4 - 5 * (unit >> 4) - low)
    return z, slot


def remote(src, dst, send, recv, device):
    return pltpu.make_async_remote_copy(
        src_ref=src,
        dst_ref=dst,
        send_sem=send,
        recv_sem=recv,
        device_id=device,
        device_id_type=pl.DeviceIdType.MESH,
    )


def cols(slot):
    return pl.ds(pl.multiple_of(slot * UNIT, UNIT), UNIT)


def greet(devices):
    barrier = pltpu.get_barrier_semaphore()
    for device in devices:
        pl.semaphore_signal(barrier, inc=1, device_id=device, device_id_type=pl.DeviceIdType.MESH)
    pl.semaphore_wait(barrier, len(devices))


def fused_kernel(
    x_ref, g_ref, p_ref, out_c, out_q, out_kv,
    xg, xt, gd, pg, kp, qp, kf, qf, kl, kr, ql, qr, kv, cp, ca, cb,
    gs1, gs, gr, ps1, ps, pr, xs, xr,
    fks, fkr, fqs, fqr, ks, kvr, qs, qvr, ss, sr, cs, crv,
):
    me = Place()
    tokens = g_ref.shape[0]
    rows = p_ref.shape[0]
    half = rows // 2
    yp, ym, yo = (me.y + 1) % 4, (me.y + 3) % 4, (me.y + 2) % 4
    xp, xm, xo = (me.x + 1) % 4, (me.x + 3) % 4, (me.x + 2) % 4
    devices = []
    for step in range(1, 8):
        far = (me.zh * 4 + me.z + step) % 8
        devices.append(me.at(z=far % 4, zh=far // 4))
    devices += [me.at(y=yp), me.at(y=ym), me.at(c=1 - me.c), me.at(x=xp), me.at(x=xm)]
    greet(devices)

    def mine(z):
        return pl.ds(pl.multiple_of(z * tokens, tokens), tokens)

    def wait_for(part, sem):
        pltpu.make_async_copy(part, part, sem).wait()

    for k in range(5):
        q, slot = slot_of(5 * me.owner + k)
        src = g_ref.at[:, k * UNIT : (k + 1) * UNIT]
        dst = gd.at[mine(me.z), cols(slot)]
        for zh in range(2):
            here = jnp.logical_and(q == me.z, me.zh == zh)

            @pl.when(here)
            def _():
                pltpu.make_async_copy(src, dst, gr.at[slot, me.z]).start()

            @pl.when(jnp.logical_not(here))
            def _():
                remote(src, dst, gs1.at[k, zh], gr.at[slot, me.z], me.at(z=q, zh=zh)).start()

    for k in range(5):
        q, slot = slot_of(5 * me.dp + k)
        src = p_ref.at[:, k * UNIT : (k + 1) * UNIT]
        dst = pg.at[:, cols(slot)]

        @pl.when(q == me.z)
        def _():
            pltpu.make_async_copy(src, dst, pr.at[slot, 0]).start()

        @pl.when(q != me.z)
        def _():
            remote(src, dst, ps1.at[k], pr.at[slot, 0], me.at(z=q)).start()

    def x_send(src, origin, side):
        to = me.z + 1 if side == 0 else me.z - 1
        return remote(src, xg.at[mine(origin)], xs.at[side, origin], xr.at[origin], me.at(z=to))

    own_x = pltpu.make_async_copy(x_ref, xg.at[mine(me.z)], xr.at[me.z])
    own_x.start()

    @pl.when(me.z < 3)
    def _():
        x_send(x_ref, me.z, 0).start()

    @pl.when(me.z > 0)
    def _():
        x_send(x_ref, me.z, 1).start()

    own_x.wait()

    def x_step(step):
        low = me.z - step
        high = me.z + step

        @pl.when(low >= 0)
        def _():
            slot = jnp.maximum(low, 0)
            block = xg.at[mine(slot)]
            wait_for(block, xr.at[slot])

            @pl.when(me.z < 3)
            def _():
                x_send(block, slot, 0).start()

        @pl.when(high <= 3)
        def _():
            slot = jnp.minimum(high, 3)
            block = xg.at[mine(slot)]
            wait_for(block, xr.at[slot])

            @pl.when(me.z > 0)
            def _():
                x_send(block, slot, 1).start()

    def g_unit(y, c, zh, k):
        q, slot = slot_of(5 * (8 * zh + 2 * y + c) + k)
        whole = gd.at[:, cols(slot)]
        upper = gd.at[0 : 2 * tokens, cols(slot)]
        lower = gd.at[2 * tokens : 4 * tokens, cols(slot)]
        return q == me.z, slot, whole, upper, lower

    def g_send(part, slot, way, index=0):
        device = (me.at(y=yp), me.at(y=ym), me.at(c=1 - me.c))[way]
        return remote(part, part, gs.at[slot, way], gr.at[slot, index], device)

    def p_unit(x, z, k):
        q, slot = slot_of(5 * (4 * x + z) + k)
        whole = pg.at[:, cols(slot)]
        upper = pg.at[0:half, cols(slot)]
        lower = pg.at[half:rows, cols(slot)]
        return q == me.z, slot, whole, upper, lower

    def p_send(part, slot, way, index=0):
        device = (me.at(x=xp), me.at(x=xm))[way]
        return remote(part, part, ps.at[slot, way], pr.at[slot, index], device)

    def g_origin(k, waiting):
        for zh in range(2):
            ok, slot, whole, upper, lower = g_unit(me.y, me.c, zh, k)

            @pl.when(ok)
            def _():
                if waiting:
                    for way in range(3):
                        wait_for(whole, gs.at[slot, way])
                else:
                    for t in range(4):
                        wait_for(gd.at[t * tokens : (t + 1) * tokens, cols(slot)], gr.at[slot, t])
                    for way in range(3):
                        g_send(whole, slot, way).start()

    def g_next(k, waiting):
        for zh in range(2):
            for side, y in ((0, ym), (1, yp)):
                ok, slot, whole, upper, lower = g_unit(y, me.c, zh, k)
                part = upper if side == 0 else lower

                @pl.when(ok)
                def _():
                    if waiting:
                        wait_for(part, gs.at[slot, side])
                        wait_for(whole, gs.at[slot, 2])
                    else:
                        wait_for(whole, gr.at[slot, 0])
                        g_send(part, slot, side, side).start()
                        g_send(whole, slot, 2).start()

    def g_last(k, waiting):
        for zh in range(2):
            ok, slot, whole, upper, lower = g_unit(yo, me.c, zh, k)

            @pl.when(ok)
            def _():
                if waiting:
                    wait_for(whole, gs.at[slot, 2])
                else:
                    wait_for(upper, gr.at[slot, 0])
                    wait_for(lower, gr.at[slot, 1])
                    g_send(whole, slot, 2).start()

    def g_sibling(k):
        for zh in range(2):
            for y in range(4):
                ok, slot, whole, upper, lower = g_unit(y, 1 - me.c, zh, k)

                @pl.when(ok)
                def _():
                    wait_for(whole, gr.at[slot, 0])

    def p_origin(k, waiting):
        for z in range(4):
            ok, slot, whole, upper, lower = p_unit(me.x, z, k)

            @pl.when(ok)
            def _():
                if waiting:
                    for way in range(2):
                        wait_for(whole, ps.at[slot, way])
                else:
                    wait_for(whole, pr.at[slot, 0])
                    for way in range(2):
                        p_send(whole, slot, way).start()

    def p_next(k, waiting):
        for z in range(4):
            for side, x in ((0, xm), (1, xp)):
                ok, slot, whole, upper, lower = p_unit(x, z, k)
                part = upper if side == 0 else lower

                @pl.when(ok)
                def _():
                    if waiting:
                        wait_for(part, ps.at[slot, side])
                    else:
                        wait_for(whole, pr.at[slot, 0])
                        p_send(part, slot, side, side).start()

    def p_last(k):
        for z in range(4):
            ok, slot, whole, upper, lower = p_unit(xo, z, k)

            @pl.when(ok)
            def _():
                wait_for(upper, pr.at[slot, 0])
                wait_for(lower, pr.at[slot, 1])

    @pl.loop(0, 5)
    def _(k):
        g_origin(k, False)

    @pl.loop(0, 5)
    def _(k):
        p_origin(k, False)
        g_next(k, False)

    x_step(1)

    @pl.loop(0, 5)
    def _(k):
        p_next(k, False)
        g_last(k, False)

    x_step(2)

    x_step(3)

    @pl.loop(0, 4)
    def _(t):
        xt[:, mine(t)] = xg[mine(t), :].T

    @pl.loop(0, 5)
    def _(k):
        g_sibling(k)

    @pl.loop(0, 5)
    def _(k):
        p_last(k)

    def w_dot(x, first, count):
        at = pl.ds(pl.multiple_of((5 * x + first) * UNIT, UNIT), count * UNIT)
        return mm(xt[...], gd[:, at])

    def c_dot(d):
        cp[d] = lax.dot_general(
            gd[mine(d), :], pg[...], (((1,), (1,)), ((), ())), preferred_element_type=F32
        ).astype(BF16)

    def add(a, b):
        return (a.astype(F32) + b.astype(F32)).astype(BF16)

    kp[0] = w_dot(xo, 4, 1).astype(BF16)
    kp[1] = w_dot(xp, 4, 1).astype(BF16)
    kp[2] = w_dot(xm, 4, 1).astype(BF16)
    plus, minus = me.at(x=xp), me.at(x=xm)
    raw_k = [
        remote(kp.at[0, 0:half], kf.at[0], fks.at[0], fkr.at[0], plus),
        remote(kp.at[0, half:rows], kf.at[1], fks.at[1], fkr.at[1], minus),
    ]
    own_k = [
        remote(kp.at[1, half:rows], kl.at[half:rows], ks.at[0], kvr.at[0], plus),
        remote(kp.at[2, 0:half], kr.at[0:half], ks.at[1], kvr.at[1], minus),
    ]
    for copy in raw_k + own_k:
        copy.start()
    qp[0] = w_dot(xo, 0, 4).astype(BF16)
    raw_q = [
        remote(qp.at[0, 0:half], qf.at[0], fqs.at[0], fqr.at[0], plus),
        remote(qp.at[0, half:rows], qf.at[1], fqs.at[1], fqr.at[1], minus),
    ]
    for copy in raw_q:
        copy.start()

    odd = me.z % 2
    near = me.at(z=me.z + 1 - 2 * odd)
    away = (me.z + 2) % 4
    c_near = []
    for part in range(2):
        d = 1 - odd + 2 * part
        c_dot(d)
        copy = remote(cp.at[d], ca.at[part], cs.at[part], crv.at[part], near)
        copy.start()
        c_near.append(copy)

    qp[1] = w_dot(xp, 0, 4).astype(BF16)
    qp[2] = w_dot(xm, 0, 4).astype(BF16)
    for copy in raw_k:
        copy.wait_recv()
    kf[0] = add(kf[0], kp[1, 0:half])
    kf[1] = add(kf[1], kp[2, half:rows])
    sum_k = [
        remote(kf.at[0], kl.at[0:half], ks.at[2], kvr.at[2], plus),
        remote(kf.at[1], kr.at[half:rows], ks.at[3], kvr.at[3], minus),
    ]
    own_q = [
        remote(qp.at[1, half:rows], ql.at[half:rows], qs.at[0], qvr.at[0], plus),
        remote(qp.at[2, 0:half], qr.at[0:half], qs.at[1], qvr.at[1], minus),
    ]
    for copy in sum_k + own_q:
        copy.start()
    c_dot(odd)
    c_dot(odd + 2)
    for copy in raw_q:
        copy.wait_recv()
    qf[0] = add(qf[0], qp[1, 0:half])
    qf[1] = add(qf[1], qp[2, half:rows])
    sum_q = [
        remote(qf.at[0], ql.at[0:half], qs.at[2], qvr.at[2], plus),
        remote(qf.at[1], qr.at[half:rows], qs.at[3], qvr.at[3], minus),
    ]
    for copy in sum_q:
        copy.start()

    kw = w_dot(me.x, 4, 1)
    for copy in own_k + sum_k:
        copy.wait_recv()
    kv[me.z] = (kw + kl[...].astype(F32) + kr[...].astype(F32)).astype(BF16)

    def kv_send(origin, side):
        to = me.z + 1 if side == 0 else me.z - 1
        return remote(kv.at[origin], kv.at[origin], ss.at[side, origin], sr.at[origin], me.at(z=to))

    @pl.when(me.z < 3)
    def _():
        kv_send(me.z, 0).start()

    @pl.when(me.z > 0)
    def _():
        kv_send(me.z, 1).start()

    for copy in c_near:
        copy.wait_recv()
    cb[0] = add(cp[away], ca[away // 2])
    c_far = remote(cb.at[0], cb.at[1], cs.at[2], crv.at[2], me.at(z=away))
    c_far.start()
    qw = w_dot(me.x, 0, 4)

    for step in range(1, 4):
        low = me.z - step
        high = me.z + step

        @pl.when(low >= 0)
        def _():
            slot = jnp.maximum(low, 0)
            wait_for(kv.at[slot], sr.at[slot])

            @pl.when(me.z < 3)
            def _():
                kv_send(slot, 0).start()

        @pl.when(high <= 3)
        def _():
            slot = jnp.minimum(high, 3)
            wait_for(kv.at[slot], sr.at[slot])

            @pl.when(me.z > 0)
            def _():
                kv_send(slot, 1).start()

    gram = left_of(kv[0])
    for part in range(1, 4):
        gram += left_of(kv[part])
    out_kv[...] = update_of(gram, kv[me.z])

    for copy in own_q + sum_q:
        copy.wait_recv()
    square = (qw + ql[...].astype(F32) + qr[...].astype(F32)).astype(BF16)
    out_q[...] = update_of(left_of(square), square)

    c_far.wait_recv()
    out_c[...] = (
        cp[me.z].astype(F32) + ca[me.z // 2].astype(F32) + cb[1].astype(F32)
    ).astype(BF16)

    for k in range(5):
        q, slot = slot_of(5 * me.owner + k)
        src = g_ref.at[:, k * UNIT : (k + 1) * UNIT]
        for zh in range(2):
            @pl.when(jnp.logical_not(jnp.logical_and(q == me.z, me.zh == zh)))
            def _():
                wait_for(src, gs1.at[k, zh])

        q, slot = slot_of(5 * me.dp + k)
        psrc = p_ref.at[:, k * UNIT : (k + 1) * UNIT]

        @pl.when(q != me.z)
        def _():
            wait_for(psrc, ps1.at[k])

    @pl.loop(0, 5)
    def _(k):
        g_origin(k, True)
        g_next(k, True)
        g_last(k, True)
        p_origin(k, True)
        p_next(k, True)

    for origin in range(4):
        block = xg.at[origin * tokens : (origin + 1) * tokens]

        @pl.when(jnp.logical_and(origin <= me.z, me.z < 3))
        def _():
            wait_for(block, xs.at[0, origin])
            wait_for(kv.at[origin], ss.at[0, origin])

        @pl.when(jnp.logical_and(origin >= me.z, me.z > 0))
        def _():
            wait_for(block, xs.at[1, origin])
            wait_for(kv.at[origin], ss.at[1, origin])

    for copy in raw_k + own_k + sum_k + raw_q + own_q + sum_q + c_near + [c_far]:
        copy.wait_send()


def dma(*shape):
    return pltpu.SemaphoreType.DMA(shape)


def split(value):
    high = value.astype(BF16)
    return high, (value - high.astype(F32)).astype(BF16)


def mm(a, b):
    return lax.dot_general(a, b, (((1,), (0,)), ((), ())), preferred_element_type=F32)


def update_of(left, target):
    width = left.shape[0]
    scale = math.sqrt(width) * jnp.sqrt(jnp.mean(left * left) + 1e-06)
    lh, ll = split(left * (1.0 / scale))
    once = mm(lh, target) + mm(ll, target)
    oh, ol = split(once)
    twice = mm(lh, oh) + mm(ll, oh) + mm(lh, ol)
    factor = math.sqrt(width) / 16.0 * lax.rsqrt(scale)
    return (factor * (25.0 * target.astype(F32) - 10.0 * once + twice)).astype(BF16)


def left_of(block):
    return lax.dot_general(block, block, (((1,), (1,)), ((), ())), preferred_element_type=F32)


def body(layer_input, output_grads, projection):
    tokens, rows = layer_input.shape
    half = rows // 2
    shape = jax.ShapeDtypeStruct
    vmem = pl.BlockSpec(memory_space=pltpu.VMEM)

    def space(*dims):
        return pltpu.VMEM(dims, BF16)

    return pl.pallas_call(
        fused_kernel,
        name="fused",
        out_shape=(
            shape((tokens, rows), BF16),
            shape((rows, BLOCK), BF16),
            shape((rows, UNIT), BF16),
        ),
        in_specs=[pl.BlockSpec(memory_space=pl.ANY)] * 3,
        out_specs=(vmem, vmem, vmem),
        scratch_shapes=[
            space(4 * tokens, rows),
            space(rows, 4 * tokens),
            space(4 * tokens, SLOTS * UNIT),
            space(rows, SLOTS * UNIT),
            space(3, rows, UNIT),
            space(3, rows, BLOCK),
            space(2, half, UNIT),
            space(2, half, BLOCK),
            space(rows, UNIT),
            space(rows, UNIT),
            space(rows, BLOCK),
            space(rows, BLOCK),
            space(4, rows, UNIT),
            space(4, tokens, rows),
            space(2, tokens, rows),
            space(2, tokens, rows),
            dma(5, 2),
            dma(SLOTS, 3),
            dma(SLOTS, 4),
            dma(5),
            dma(SLOTS, 2),
            dma(SLOTS, 2),
            dma(2, 4),
            dma(4),
            dma(2),
            dma(2),
            dma(2),
            dma(2),
            dma(4),
            dma(4),
            dma(4),
            dma(4),
            dma(2, 4),
            dma(4),
            dma(3),
            dma(3),
        ],
        compiler_params=pltpu.CompilerParams(
            collective_id=0, has_side_effects=True, vmem_limit_bytes=VMEM_LIMIT
        ),
    )(layer_input, output_grads, projection)


def solution(mesh):
    placed = (P("dp", "owner"), P("dp", "owner"), P("owner", "dp"))
    return jax.shard_map(
        body,
        mesh=mesh,
        in_specs=placed,
        out_specs=(P("dp", "owner"), P("owner", "dp"), P("owner", "dp")),
        check_vma=False,
    )
```

```python
import math

import jax
import jax.numpy as jnp
from jax import lax
from jax.experimental import pallas as pl
from jax.experimental.pallas import tpu as pltpu
from jax.sharding import PartitionSpec as P

BLOCK = 512
UNIT = 128
SLOTS = 20
VMEM_LIMIT = 60 * 1024 * 1024
BF16 = jnp.bfloat16
F32 = jnp.float32


class Place:
    def __init__(self):
        dp = lax.axis_index("dp")
        owner = lax.axis_index("owner")
        self.x = dp >> 2
        self.z = dp & 3
        self.zh = owner >> 3
        self.y = (owner >> 1) & 3
        self.c = owner & 1
        self.dp = dp
        self.owner = owner

    def at(self, x=None, z=None, zh=None, y=None, c=None):
        x = self.x if x is None else x
        z = self.z if z is None else z
        zh = self.zh if zh is None else zh
        y = self.y if y is None else y
        c = self.c if c is None else c
        return (x * 4 + z, zh * 8 + y * 2 + c)


def unit_of(z, slot):
    group = slot // 5
    step = slot % 5
    kv = step // 4
    return (1 - kv) * (16 * group + 4 * z + step) + kv * (64 + 4 * group + z)


def slot_of(unit):
    kv = unit >> 6
    group = unit >> 2
    low = unit - (group << 2)
    rest = group & 3
    z = rest + kv * (low - rest)
    slot = 5 * (unit >> 4) + low + kv * (5 * (group - 16) + 4 - 5 * (unit >> 4) - low)
    return z, slot


def remote(src, dst, send, recv, device):
    return pltpu.make_async_remote_copy(
        src_ref=src,
        dst_ref=dst,
        send_sem=send,
        recv_sem=recv,
        device_id=device,
        device_id_type=pl.DeviceIdType.MESH,
    )


def cols(slot):
    return pl.ds(pl.multiple_of(slot * UNIT, UNIT), UNIT)


def greet(devices):
    barrier = pltpu.get_barrier_semaphore()
    for device in devices:
        pl.semaphore_signal(barrier, inc=1, device_id=device, device_id_type=pl.DeviceIdType.MESH)
    pl.semaphore_wait(barrier, len(devices))


def fused_kernel(
    x_ref, g_ref, p_ref, out_c, out_q, out_kv, pin,
    xg, xt, gd, pg, kp, qp, kf, qf, kl, kr, ql, qr, kv, cp, ca, cb,
    gs1, gs, gr, p0s, p0r, p1s, p1r, ps, pf, pr, pl_sem, xs, xr,
    fks, fkr, fqs, fqr, ks, kvr, qs, qvr, ss, sr, cs, crv,
):
    me = Place()
    tokens = g_ref.shape[0]
    rows = p_ref.shape[0]
    half = rows // 2
    yp, ym, yo = (me.y + 1) % 4, (me.y + 3) % 4, (me.y + 2) % 4
    xp, xm, xo = (me.x + 1) % 4, (me.x + 3) % 4, (me.x + 2) % 4
    devices = []
    for step in range(1, 8):
        far = (me.zh * 4 + me.z + step) % 8
        devices.append(me.at(z=far % 4, zh=far // 4))
    devices += [me.at(y=yp), me.at(y=ym), me.at(c=1 - me.c), me.at(x=xp), me.at(x=xm), me.at(x=xo)]
    greet(devices)

    def mine(z):
        return pl.ds(pl.multiple_of(z * tokens, tokens), tokens)

    def wait_for(part, sem):
        pltpu.make_async_copy(part, part, sem).wait()

    quarter = rows // 4
    width = p_ref.shape[1]

    def share(x):
        return pl.ds(pl.multiple_of(x * quarter, quarter), quarter)

    def group_cols(group):
        return pl.ds(pl.multiple_of(group * width, UNIT), width)

    scatter = []
    for step, x in ((1, xp), (3, xm), (2, xo)):
        copy = remote(
            p_ref.at[share(x)], pin.at[me.x], p0s.at[step], p0r.at[me.x], me.at(x=x)
        )
        copy.start()
        scatter.append(copy)

    for k in range(5):
        q, slot = slot_of(5 * me.owner + k)
        src = g_ref.at[:, k * UNIT : (k + 1) * UNIT]
        dst = gd.at[mine(me.z), cols(slot)]
        for zh in range(2):
            here = jnp.logical_and(q == me.z, me.zh == zh)

            @pl.when(here)
            def _():
                pltpu.make_async_copy(src, dst, gr.at[slot, me.z]).start()

            @pl.when(jnp.logical_not(here))
            def _():
                remote(src, dst, gs1.at[k, zh], gr.at[slot, me.z], me.at(z=q, zh=zh)).start()

    def x_send(src, origin, side):
        to = me.z + 1 if side == 0 else me.z - 1
        return remote(src, xg.at[mine(origin)], xs.at[side, origin], xr.at[origin], me.at(z=to))

    def quarter_unit(x, step, k):
        unit = 5 * (4 * x + me.z) + k
        q, slot = slot_of(unit)
        kv_unit = unit >> 6
        group = (unit >> 4) + kv_unit * ((unit >> 2) - 16 - (unit >> 4))
        at = slice(k * UNIT, (k + 1) * UNIT)
        src = p_ref.at[share(me.x), at] if step == 0 else pin.at[x, :, at]
        return q, src, pg.at[share(me.x), cols(slot)], group

    quarters = ((0, me.x), (1, xm), (3, xp), (2, xo))
    for step, x in quarters:
        if step:
            wait_for(pin.at[x], p0r.at[x])
        for k in range(5):
            q, src, dst, group = quarter_unit(x, step, k)

            @pl.when(q == me.z)
            def _():
                pltpu.make_async_copy(src, dst, p1r.at[group]).start()

            @pl.when(q != me.z)
            def _():
                remote(src, dst, p1s.at[step, k], p1r.at[group], me.at(z=q)).start()

    own_x = pltpu.make_async_copy(x_ref, xg.at[mine(me.z)], xr.at[me.z])
    own_x.start()

    @pl.when(me.z < 3)
    def _():
        x_send(x_ref, me.z, 0).start()

    @pl.when(me.z > 0)
    def _():
        x_send(x_ref, me.z, 1).start()

    own_x.wait()

    def x_step(step):
        low = me.z - step
        high = me.z + step

        @pl.when(low >= 0)
        def _():
            slot = jnp.maximum(low, 0)
            block = xg.at[mine(slot)]
            wait_for(block, xr.at[slot])

            @pl.when(me.z < 3)
            def _():
                x_send(block, slot, 0).start()

        @pl.when(high <= 3)
        def _():
            slot = jnp.minimum(high, 3)
            block = xg.at[mine(slot)]
            wait_for(block, xr.at[slot])

            @pl.when(me.z > 0)
            def _():
                x_send(block, slot, 1).start()

    def g_unit(y, c, zh, k):
        q, slot = slot_of(5 * (8 * zh + 2 * y + c) + k)
        whole = gd.at[:, cols(slot)]
        upper = gd.at[0 : 2 * tokens, cols(slot)]
        lower = gd.at[2 * tokens : 4 * tokens, cols(slot)]
        return q == me.z, slot, whole, upper, lower

    def g_send(part, slot, way, index=0):
        device = (me.at(y=yp), me.at(y=ym), me.at(c=1 - me.c))[way]
        return remote(part, part, gs.at[slot, way], gr.at[slot, index], device)

    def p_block(x, group):
        start = x * quarter
        middle = quarter // 2
        whole = pg.at[share(x), group_cols(group)]
        upper = pg.at[pl.ds(pl.multiple_of(start, middle), middle), group_cols(group)]
        lower = pg.at[pl.ds(pl.multiple_of(start + middle, middle), middle), group_cols(group)]
        return whole, upper, lower

    def g_origin(k, waiting):
        for zh in range(2):
            ok, slot, whole, upper, lower = g_unit(me.y, me.c, zh, k)

            @pl.when(ok)
            def _():
                if waiting:
                    for way in range(3):
                        wait_for(whole, gs.at[slot, way])
                else:
                    for t in range(4):
                        wait_for(gd.at[t * tokens : (t + 1) * tokens, cols(slot)], gr.at[slot, t])
                    for way in range(3):
                        g_send(whole, slot, way).start()

    def g_next(k, waiting):
        for zh in range(2):
            for side, y in ((0, ym), (1, yp)):
                ok, slot, whole, upper, lower = g_unit(y, me.c, zh, k)
                part = upper if side == 0 else lower

                @pl.when(ok)
                def _():
                    if waiting:
                        wait_for(part, gs.at[slot, side])
                        wait_for(whole, gs.at[slot, 2])
                    else:
                        wait_for(whole, gr.at[slot, 0])
                        g_send(part, slot, side, side).start()
                        g_send(whole, slot, 2).start()

    def g_last(k, waiting):
        for zh in range(2):
            ok, slot, whole, upper, lower = g_unit(yo, me.c, zh, k)

            @pl.when(ok)
            def _():
                if waiting:
                    wait_for(whole, gs.at[slot, 2])
                else:
                    wait_for(upper, gr.at[slot, 0])
                    wait_for(lower, gr.at[slot, 1])
                    g_send(whole, slot, 2).start()

    def g_sibling(k):
        for zh in range(2):
            for y in range(4):
                ok, slot, whole, upper, lower = g_unit(y, 1 - me.c, zh, k)

                @pl.when(ok)
                def _():
                    wait_for(whole, gr.at[slot, 0])

    def p_origin(group):
        whole, upper, lower = p_block(me.x, group)
        wait_for(whole, p1r.at[group])
        for way, x in ((0, xp), (1, xm)):
            remote(whole, whole, ps.at[way, group], pr.at[me.x, group], me.at(x=x)).start()

    def p_next(group):
        whole, upper, lower = p_block(xm, group)
        wait_for(whole, pr.at[xm, group])
        remote(upper, upper, pf.at[0, group], pr.at[xm, group], me.at(x=xp)).start()
        whole, upper, lower = p_block(xp, group)
        wait_for(whole, pr.at[xp, group])
        remote(lower, lower, pf.at[1, group], pl_sem.at[group], me.at(x=xm)).start()

    def p_last(group):
        whole, upper, lower = p_block(xo, group)
        wait_for(upper, pr.at[xo, group])
        wait_for(lower, pl_sem.at[group])

    def p_sent(group):
        for way in range(2):
            wait_for(p_block(me.x, group)[0], ps.at[way, group])
        wait_for(p_block(xm, group)[1], pf.at[0, group])
        wait_for(p_block(xp, group)[2], pf.at[1, group])

    @pl.loop(0, 5)
    def _(k):
        g_origin(k, False)

    @pl.loop(0, 5)
    def _(k):
        g_next(k, False)

        @pl.when(k < 4)
        def _():
            p_origin(k)


    x_step(1)

    @pl.loop(0, 5)
    def _(k):
        g_last(k, False)

        @pl.when(k < 4)
        def _():
            p_next(k)


    x_step(2)

    x_step(3)

    @pl.loop(0, 4)
    def _(t):
        xt[:, mine(t)] = xg[mine(t), :].T

    @pl.loop(0, 5)
    def _(k):
        g_sibling(k)

    @pl.loop(0, 4)
    def _(group):
        p_last(group)

    def w_dot(x, first, count):
        at = pl.ds(pl.multiple_of((5 * x + first) * UNIT, UNIT), count * UNIT)
        return mm(xt[...], gd[:, at])

    def c_dot(d):
        cp[d] = lax.dot_general(
            gd[mine(d), :], pg[...], (((1,), (1,)), ((), ())), preferred_element_type=F32
        ).astype(BF16)

    def add(a, b):
        return (a.astype(F32) + b.astype(F32)).astype(BF16)

    kp[0] = w_dot(xo, 4, 1).astype(BF16)
    kp[1] = w_dot(xp, 4, 1).astype(BF16)
    kp[2] = w_dot(xm, 4, 1).astype(BF16)
    plus, minus = me.at(x=xp), me.at(x=xm)
    raw_k = [
        remote(kp.at[0, 0:half], kf.at[0], fks.at[0], fkr.at[0], plus),
        remote(kp.at[0, half:rows], kf.at[1], fks.at[1], fkr.at[1], minus),
    ]
    own_k = [
        remote(kp.at[1, half:rows], kl.at[half:rows], ks.at[0], kvr.at[0], plus),
        remote(kp.at[2, 0:half], kr.at[0:half], ks.at[1], kvr.at[1], minus),
    ]
    for copy in raw_k + own_k:
        copy.start()
    qp[0] = w_dot(xo, 0, 4).astype(BF16)
    raw_q = [
        remote(qp.at[0, 0:half], qf.at[0], fqs.at[0], fqr.at[0], plus),
        remote(qp.at[0, half:rows], qf.at[1], fqs.at[1], fqr.at[1], minus),
    ]
    for copy in raw_q:
        copy.start()

    odd = me.z % 2
    near = me.at(z=me.z + 1 - 2 * odd)
    away = (me.z + 2) % 4
    c_near = []
    for part in range(2):
        d = 1 - odd + 2 * part
        c_dot(d)
        copy = remote(cp.at[d], ca.at[part], cs.at[part], crv.at[part], near)
        copy.start()
        c_near.append(copy)

    qp[1] = w_dot(xp, 0, 4).astype(BF16)
    qp[2] = w_dot(xm, 0, 4).astype(BF16)
    for copy in raw_k:
        copy.wait_recv()
    kf[0] = add(kf[0], kp[1, 0:half])
    kf[1] = add(kf[1], kp[2, half:rows])
    sum_k = [
        remote(kf.at[0], kl.at[0:half], ks.at[2], kvr.at[2], plus),
        remote(kf.at[1], kr.at[half:rows], ks.at[3], kvr.at[3], minus),
    ]
    own_q = [
        remote(qp.at[1, half:rows], ql.at[half:rows], qs.at[0], qvr.at[0], plus),
        remote(qp.at[2, 0:half], qr.at[0:half], qs.at[1], qvr.at[1], minus),
    ]
    for copy in sum_k + own_q:
        copy.start()
    c_dot(odd)
    c_dot(odd + 2)
    for copy in raw_q:
        copy.wait_recv()
    qf[0] = add(qf[0], qp[1, 0:half])
    qf[1] = add(qf[1], qp[2, half:rows])
    sum_q = [
        remote(qf.at[0], ql.at[0:half], qs.at[2], qvr.at[2], plus),
        remote(qf.at[1], qr.at[half:rows], qs.at[3], qvr.at[3], minus),
    ]
    for copy in sum_q:
        copy.start()

    kw = w_dot(me.x, 4, 1)
    for copy in own_k + sum_k:
        copy.wait_recv()
    kv[me.z] = (kw + kl[...].astype(F32) + kr[...].astype(F32)).astype(BF16)

    def kv_send(origin, side):
        to = me.z + 1 if side == 0 else me.z - 1
        return remote(kv.at[origin], kv.at[origin], ss.at[side, origin], sr.at[origin], me.at(z=to))

    @pl.when(me.z < 3)
    def _():
        kv_send(me.z, 0).start()

    @pl.when(me.z > 0)
    def _():
        kv_send(me.z, 1).start()

    for copy in c_near:
        copy.wait_recv()
    cb[0] = add(cp[away], ca[away // 2])
    c_far = remote(cb.at[0], cb.at[1], cs.at[2], crv.at[2], me.at(z=away))
    c_far.start()
    qw = w_dot(me.x, 0, 4)

    for step in range(1, 4):
        low = me.z - step
        high = me.z + step

        @pl.when(low >= 0)
        def _():
            slot = jnp.maximum(low, 0)
            wait_for(kv.at[slot], sr.at[slot])

            @pl.when(me.z < 3)
            def _():
                kv_send(slot, 0).start()

        @pl.when(high <= 3)
        def _():
            slot = jnp.minimum(high, 3)
            wait_for(kv.at[slot], sr.at[slot])

            @pl.when(me.z > 0)
            def _():
                kv_send(slot, 1).start()

    gram = left_of(kv[0])
    for part in range(1, 4):
        gram += left_of(kv[part])
    out_kv[...] = update_of(gram, kv[me.z])

    for copy in own_q + sum_q:
        copy.wait_recv()
    square = (qw + ql[...].astype(F32) + qr[...].astype(F32)).astype(BF16)
    out_q[...] = update_of(left_of(square), square)

    c_far.wait_recv()
    out_c[...] = (
        cp[me.z].astype(F32) + ca[me.z // 2].astype(F32) + cb[1].astype(F32)
    ).astype(BF16)

    for k in range(5):
        q, slot = slot_of(5 * me.owner + k)
        src = g_ref.at[:, k * UNIT : (k + 1) * UNIT]
        for zh in range(2):
            @pl.when(jnp.logical_not(jnp.logical_and(q == me.z, me.zh == zh)))
            def _():
                wait_for(src, gs1.at[k, zh])

    for step, x in quarters:
        for k in range(5):
            q, src, dst, group = quarter_unit(x, step, k)

            @pl.when(q != me.z)
            def _():
                wait_for(src, p1s.at[step, k])

    @pl.loop(0, 4)
    def _(group):
        p_sent(group)

    @pl.loop(0, 5)
    def _(k):
        g_origin(k, True)
        g_next(k, True)
        g_last(k, True)

    for origin in range(4):
        block = xg.at[origin * tokens : (origin + 1) * tokens]

        @pl.when(jnp.logical_and(origin <= me.z, me.z < 3))
        def _():
            wait_for(block, xs.at[0, origin])
            wait_for(kv.at[origin], ss.at[0, origin])

        @pl.when(jnp.logical_and(origin >= me.z, me.z > 0))
        def _():
            wait_for(block, xs.at[1, origin])
            wait_for(kv.at[origin], ss.at[1, origin])

    for copy in raw_k + own_k + sum_k + raw_q + own_q + sum_q + c_near + [c_far] + scatter:
        copy.wait_send()


def dma(*shape):
    return pltpu.SemaphoreType.DMA(shape)


def split(value):
    high = value.astype(BF16)
    return high, (value - high.astype(F32)).astype(BF16)


def mm(a, b):
    return lax.dot_general(a, b, (((1,), (0,)), ((), ())), preferred_element_type=F32)


def update_of(left, target):
    width = left.shape[0]
    scale = math.sqrt(width) * jnp.sqrt(jnp.mean(left * left) + 1e-06)
    lh, ll = split(left * (1.0 / scale))
    once = mm(lh, target) + mm(ll, target)
    oh, ol = split(once)
    twice = mm(lh, oh) + mm(ll, oh) + mm(lh, ol)
    factor = math.sqrt(width) / 16.0 * lax.rsqrt(scale)
    return (factor * (25.0 * target.astype(F32) - 10.0 * once + twice)).astype(BF16)


def left_of(block):
    return lax.dot_general(block, block, (((1,), (1,)), ((), ())), preferred_element_type=F32)


def body(layer_input, output_grads, projection):
    tokens, rows = layer_input.shape
    half = rows // 2
    shape = jax.ShapeDtypeStruct
    vmem = pl.BlockSpec(memory_space=pltpu.VMEM)

    def space(*dims):
        return pltpu.VMEM(dims, BF16)

    return pl.pallas_call(
        fused_kernel,
        name="fused",
        out_shape=(
            shape((tokens, rows), BF16),
            shape((rows, BLOCK), BF16),
            shape((rows, UNIT), BF16),
            shape((4, rows // 4, projection.shape[1]), BF16),
        ),
        in_specs=[pl.BlockSpec(memory_space=pl.ANY)] * 3,
        out_specs=(vmem, vmem, vmem, pl.BlockSpec(memory_space=pl.ANY)),
        scratch_shapes=[
            space(4 * tokens, rows),
            space(rows, 4 * tokens),
            space(4 * tokens, SLOTS * UNIT),
            space(rows, SLOTS * UNIT),
            space(3, rows, UNIT),
            space(3, rows, BLOCK),
            space(2, half, UNIT),
            space(2, half, BLOCK),
            space(rows, UNIT),
            space(rows, UNIT),
            space(rows, BLOCK),
            space(rows, BLOCK),
            space(4, rows, UNIT),
            space(4, tokens, rows),
            space(2, tokens, rows),
            space(2, tokens, rows),
            dma(5, 2),
            dma(SLOTS, 3),
            dma(SLOTS, 4),
            dma(4),
            dma(4),
            dma(4, 5),
            dma(4),
            dma(2, 4),
            dma(2, 4),
            dma(4, 4),
            dma(4),
            dma(2, 4),
            dma(4),
            dma(2),
            dma(2),
            dma(2),
            dma(2),
            dma(4),
            dma(4),
            dma(4),
            dma(4),
            dma(2, 4),
            dma(4),
            dma(3),
            dma(3),
        ],
        compiler_params=pltpu.CompilerParams(
            collective_id=0, has_side_effects=True, vmem_limit_bytes=VMEM_LIMIT
        ),
    )(layer_input, output_grads, projection)[:3]


def solution(mesh):
    placed = (P("dp", "owner"), P("dp", "owner"), P("owner", "dp"))
    return jax.shard_map(
        body,
        mesh=mesh,
        in_specs=placed,
        out_specs=(P("dp", "owner"), P("owner", "dp"), P("owner", "dp")),
        check_vma=False,
    )
```

```python
import math

import jax
import jax.numpy as jnp
from jax import lax
from jax.experimental import pallas as pl
from jax.experimental.pallas import tpu as pltpu
from jax.sharding import PartitionSpec as P

BLOCK = 512
UNIT = 128
SLOTS = 20
VMEM_LIMIT = 60 * 1024 * 1024
BF16 = jnp.bfloat16
F32 = jnp.float32


class Place:
    def __init__(self):
        dp = lax.axis_index("dp")
        owner = lax.axis_index("owner")
        self.x = dp >> 2
        self.z = dp & 3
        self.zh = owner >> 3
        self.y = (owner >> 1) & 3
        self.c = owner & 1
        self.dp = dp
        self.owner = owner

    def at(self, x=None, z=None, zh=None, y=None, c=None):
        x = self.x if x is None else x
        z = self.z if z is None else z
        zh = self.zh if zh is None else zh
        y = self.y if y is None else y
        c = self.c if c is None else c
        return (x * 4 + z, zh * 8 + y * 2 + c)


def unit_of(z, slot):
    group = slot // 5
    step = slot % 5
    kv = step // 4
    return (1 - kv) * (16 * group + 4 * z + step) + kv * (64 + 4 * group + z)


def slot_of(unit):
    kv = unit >> 6
    group = unit >> 2
    low = unit - (group << 2)
    rest = group & 3
    z = rest + kv * (low - rest)
    slot = 5 * (unit >> 4) + low + kv * (5 * (group - 16) + 4 - 5 * (unit >> 4) - low)
    return z, slot


def remote(src, dst, send, recv, device):
    return pltpu.make_async_remote_copy(
        src_ref=src,
        dst_ref=dst,
        send_sem=send,
        recv_sem=recv,
        device_id=device,
        device_id_type=pl.DeviceIdType.MESH,
    )


def cols(slot):
    return pl.ds(pl.multiple_of(slot * UNIT, UNIT), UNIT)


def greet(devices):
    barrier = pltpu.get_barrier_semaphore()
    for device in devices:
        pl.semaphore_signal(barrier, inc=1, device_id=device, device_id_type=pl.DeviceIdType.MESH)
    pl.semaphore_wait(barrier, len(devices))


def fused_kernel(
    x_ref, g_ref, p_ref, out_kv, out_c, out_q, pin,
    xg, xt, gd, pg, kp, qp, kf, qf, kl, kr, ql, qr, kv, cp, ca, cb,
    gs1, gs, gr, p0s, p0r, p1s, p1r, ps, pf, pr, pl_sem, xs, xr,
    fks, fkr, fqs, fqr, ks, kvr, qs, qvr, ss, sr, cs, crv,
):
    me = Place()
    tokens = g_ref.shape[0]
    rows = p_ref.shape[0]
    half = rows // 2
    yp, ym, yo = (me.y + 1) % 4, (me.y + 3) % 4, (me.y + 2) % 4
    xp, xm, xo = (me.x + 1) % 4, (me.x + 3) % 4, (me.x + 2) % 4
    devices = []
    for step in range(1, 8):
        far = (me.zh * 4 + me.z + step) % 8
        devices.append(me.at(z=far % 4, zh=far // 4))
    devices += [me.at(y=yp), me.at(y=ym), me.at(c=1 - me.c), me.at(x=xp), me.at(x=xm), me.at(x=xo)]
    greet(devices)

    def mine(z):
        return pl.ds(pl.multiple_of(z * tokens, tokens), tokens)

    def wait_for(part, sem):
        pltpu.make_async_copy(part, part, sem).wait()

    quarter = rows // 4
    width = p_ref.shape[1]

    def share(x):
        return pl.ds(pl.multiple_of(x * quarter, quarter), quarter)

    def group_cols(group):
        return pl.ds(pl.multiple_of(group * width, UNIT), width)

    scatter = []
    for step, x in ((1, xp), (3, xm), (2, xo)):
        copy = remote(
            p_ref.at[share(x)], pin.at[me.x], p0s.at[step], p0r.at[me.x], me.at(x=x)
        )
        copy.start()
        scatter.append(copy)

    for k in range(5):
        q, slot = slot_of(5 * me.owner + k)
        src = g_ref.at[:, k * UNIT : (k + 1) * UNIT]
        dst = gd.at[mine(me.z), cols(slot)]
        for zh in range(2):
            here = jnp.logical_and(q == me.z, me.zh == zh)

            @pl.when(here)
            def _():
                pltpu.make_async_copy(src, dst, gr.at[slot, me.z]).start()

            @pl.when(jnp.logical_not(here))
            def _():
                remote(src, dst, gs1.at[k, zh], gr.at[slot, me.z], me.at(z=q, zh=zh)).start()

    def x_send(src, origin, side):
        to = me.z + 1 if side == 0 else me.z - 1
        return remote(src, xg.at[mine(origin)], xs.at[side, origin], xr.at[origin], me.at(z=to))

    def quarter_unit(x, step, k):
        unit = 5 * (4 * x + me.z) + k
        q, slot = slot_of(unit)
        kv_unit = unit >> 6
        group = (unit >> 4) + kv_unit * ((unit >> 2) - 16 - (unit >> 4))
        at = slice(k * UNIT, (k + 1) * UNIT)
        src = p_ref.at[share(me.x), at] if step == 0 else pin.at[x, :, at]
        return q, src, pg.at[share(me.x), cols(slot)], group

    quarters = ((0, me.x), (1, xm), (3, xp), (2, xo))
    for step, x in quarters:
        if step:
            wait_for(pin.at[x], p0r.at[x])
        for k in range(5):
            q, src, dst, group = quarter_unit(x, step, k)

            @pl.when(q == me.z)
            def _():
                pltpu.make_async_copy(src, dst, p1r.at[group]).start()

            @pl.when(q != me.z)
            def _():
                remote(src, dst, p1s.at[step, k], p1r.at[group], me.at(z=q)).start()

    own_x = pltpu.make_async_copy(x_ref, xg.at[mine(me.z)], xr.at[me.z])
    own_x.start()

    @pl.when(me.z < 3)
    def _():
        x_send(x_ref, me.z, 0).start()

    @pl.when(me.z > 0)
    def _():
        x_send(x_ref, me.z, 1).start()

    own_x.wait()

    def x_step(step):
        low = me.z - step
        high = me.z + step

        @pl.when(low >= 0)
        def _():
            slot = jnp.maximum(low, 0)
            block = xg.at[mine(slot)]
            wait_for(block, xr.at[slot])

            @pl.when(me.z < 3)
            def _():
                x_send(block, slot, 0).start()

        @pl.when(high <= 3)
        def _():
            slot = jnp.minimum(high, 3)
            block = xg.at[mine(slot)]
            wait_for(block, xr.at[slot])

            @pl.when(me.z > 0)
            def _():
                x_send(block, slot, 1).start()

    def g_unit(y, c, zh, k):
        q, slot = slot_of(5 * (8 * zh + 2 * y + c) + k)
        whole = gd.at[:, cols(slot)]
        upper = gd.at[0 : 2 * tokens, cols(slot)]
        lower = gd.at[2 * tokens : 4 * tokens, cols(slot)]
        return q == me.z, slot, whole, upper, lower

    def g_send(part, slot, way, index=0):
        device = (me.at(y=yp), me.at(y=ym), me.at(c=1 - me.c))[way]
        return remote(part, part, gs.at[slot, way], gr.at[slot, index], device)

    def p_block(x, group):
        start = x * quarter
        middle = quarter // 2
        whole = pg.at[share(x), group_cols(group)]
        upper = pg.at[pl.ds(pl.multiple_of(start, middle), middle), group_cols(group)]
        lower = pg.at[pl.ds(pl.multiple_of(start + middle, middle), middle), group_cols(group)]
        return whole, upper, lower

    def g_origin(k, waiting):
        for zh in range(2):
            ok, slot, whole, upper, lower = g_unit(me.y, me.c, zh, k)

            @pl.when(ok)
            def _():
                if waiting:
                    for way in range(3):
                        wait_for(whole, gs.at[slot, way])
                else:
                    for t in range(4):
                        wait_for(gd.at[t * tokens : (t + 1) * tokens, cols(slot)], gr.at[slot, t])
                    g_send(upper, slot, 0, 0).start()
                    g_send(lower, slot, 1, 1).start()
                    g_send(lower, slot, 0, 1).start()
                    g_send(upper, slot, 1, 0).start()
                    g_send(whole, slot, 2).start()

    def g_next(k, waiting):
        for zh in range(2):
            for side, y in ((0, ym), (1, yp)):
                ok, slot, whole, upper, lower = g_unit(y, me.c, zh, k)
                part = upper if side == 0 else lower

                @pl.when(ok)
                def _():
                    if waiting:
                        wait_for(part, gs.at[slot, side])
                        wait_for(whole, gs.at[slot, 2])
                    else:
                        rest = lower if side == 0 else upper
                        wait_for(part, gr.at[slot, side])
                        g_send(part, slot, side, side).start()
                        wait_for(rest, gr.at[slot, 1 - side])
                        g_send(whole, slot, 2).start()

    def g_last(k, waiting):
        for zh in range(2):
            ok, slot, whole, upper, lower = g_unit(yo, me.c, zh, k)

            @pl.when(ok)
            def _():
                if waiting:
                    wait_for(whole, gs.at[slot, 2])
                else:
                    wait_for(upper, gr.at[slot, 0])
                    wait_for(lower, gr.at[slot, 1])
                    g_send(whole, slot, 2).start()

    def g_sibling(k):
        for zh in range(2):
            for y in range(4):
                ok, slot, whole, upper, lower = g_unit(y, 1 - me.c, zh, k)

                @pl.when(ok)
                def _():
                    wait_for(whole, gr.at[slot, 0])

    def p_origin(group):
        whole, upper, lower = p_block(me.x, group)
        wait_for(whole, p1r.at[group])
        for way, x in ((0, xp), (1, xm)):
            remote(whole, whole, ps.at[way, group], pr.at[me.x, group], me.at(x=x)).start()

    def p_next(group):
        whole, upper, lower = p_block(xm, group)
        wait_for(whole, pr.at[xm, group])
        remote(upper, upper, pf.at[0, group], pr.at[xm, group], me.at(x=xp)).start()
        whole, upper, lower = p_block(xp, group)
        wait_for(whole, pr.at[xp, group])
        remote(lower, lower, pf.at[1, group], pl_sem.at[group], me.at(x=xm)).start()

    def p_last(group):
        whole, upper, lower = p_block(xo, group)
        wait_for(upper, pr.at[xo, group])
        wait_for(lower, pl_sem.at[group])

    def p_sent(group):
        for way in range(2):
            wait_for(p_block(me.x, group)[0], ps.at[way, group])
        wait_for(p_block(xm, group)[1], pf.at[0, group])
        wait_for(p_block(xp, group)[2], pf.at[1, group])

    @pl.loop(0, 5)
    def _(k):
        g_origin(k, False)

    @pl.loop(0, 5)
    def _(k):
        g_next(k, False)

        @pl.when(k < 4)
        def _():
            p_origin(k)


    x_step(1)

    @pl.loop(0, 5)
    def _(k):
        g_last(k, False)

        @pl.when(k < 4)
        def _():
            p_next(k)


    x_step(2)

    x_step(3)

    @pl.loop(0, 4)
    def _(t):
        xt[:, mine(t)] = xg[mine(t), :].T

    @pl.loop(0, 5)
    def _(k):
        g_sibling(k)

    @pl.loop(0, 4)
    def _(group):
        p_last(group)

    def w_dot(x, first, count):
        at = pl.ds(pl.multiple_of((5 * x + first) * UNIT, UNIT), count * UNIT)
        return mm(xt[...], gd[:, at])

    def c_dot(d):
        cp[d] = lax.dot_general(
            gd[mine(d), :], pg[...], (((1,), (1,)), ((), ())), preferred_element_type=F32
        ).astype(BF16)

    def add(a, b):
        return (a.astype(F32) + b.astype(F32)).astype(BF16)

    kp[0] = w_dot(xo, 4, 1).astype(BF16)
    kp[1] = w_dot(xp, 4, 1).astype(BF16)
    kp[2] = w_dot(xm, 4, 1).astype(BF16)
    plus, minus = me.at(x=xp), me.at(x=xm)
    raw_k = [
        remote(kp.at[0, 0:half], kf.at[0], fks.at[0], fkr.at[0], plus),
        remote(kp.at[0, half:rows], kf.at[1], fks.at[1], fkr.at[1], minus),
    ]
    own_k = [
        remote(kp.at[1, half:rows], kl.at[half:rows], ks.at[0], kvr.at[0], plus),
        remote(kp.at[2, 0:half], kr.at[0:half], ks.at[1], kvr.at[1], minus),
    ]
    for copy in raw_k + own_k:
        copy.start()
    qp[0] = w_dot(xo, 0, 4).astype(BF16)
    raw_q = [
        remote(qp.at[0, 0:half], qf.at[0], fqs.at[0], fqr.at[0], plus),
        remote(qp.at[0, half:rows], qf.at[1], fqs.at[1], fqr.at[1], minus),
    ]
    for copy in raw_q:
        copy.start()

    odd = me.z % 2
    near = me.at(z=me.z + 1 - 2 * odd)
    away = (me.z + 2) % 4
    c_near = []
    for part in range(2):
        d = 1 - odd + 2 * part
        c_dot(d)
        copy = remote(cp.at[d], ca.at[part], cs.at[part], crv.at[part], near)
        copy.start()
        c_near.append(copy)

    qp[1] = w_dot(xp, 0, 4).astype(BF16)
    qp[2] = w_dot(xm, 0, 4).astype(BF16)
    for copy in raw_k:
        copy.wait_recv()
    kf[0] = add(kf[0], kp[1, 0:half])
    kf[1] = add(kf[1], kp[2, half:rows])
    sum_k = [
        remote(kf.at[0], kl.at[0:half], ks.at[2], kvr.at[2], plus),
        remote(kf.at[1], kr.at[half:rows], ks.at[3], kvr.at[3], minus),
    ]
    own_q = [
        remote(qp.at[1, half:rows], ql.at[half:rows], qs.at[0], qvr.at[0], plus),
        remote(qp.at[2, 0:half], qr.at[0:half], qs.at[1], qvr.at[1], minus),
    ]
    for copy in sum_k + own_q:
        copy.start()
    c_dot(odd)
    c_dot(odd + 2)
    for copy in raw_q:
        copy.wait_recv()
    qf[0] = add(qf[0], qp[1, 0:half])
    qf[1] = add(qf[1], qp[2, half:rows])
    sum_q = [
        remote(qf.at[0], ql.at[0:half], qs.at[2], qvr.at[2], plus),
        remote(qf.at[1], qr.at[half:rows], qs.at[3], qvr.at[3], minus),
    ]
    for copy in sum_q:
        copy.start()

    kw = w_dot(me.x, 4, 1)
    for copy in own_k + sum_k:
        copy.wait_recv()
    kv[me.z] = (kw + kl[...].astype(F32) + kr[...].astype(F32)).astype(BF16)

    def kv_send(origin, side):
        to = me.z + 1 if side == 0 else me.z - 1
        return remote(kv.at[origin], kv.at[origin], ss.at[side, origin], sr.at[origin], me.at(z=to))

    @pl.when(me.z < 3)
    def _():
        kv_send(me.z, 0).start()

    @pl.when(me.z > 0)
    def _():
        kv_send(me.z, 1).start()

    for copy in c_near:
        copy.wait_recv()
    cb[0] = add(cp[away], ca[away // 2])
    c_far = remote(cb.at[0], cb.at[1], cs.at[2], crv.at[2], me.at(z=away))
    c_far.start()
    qw = w_dot(me.x, 0, 4)

    for step in range(1, 4):
        low = me.z - step
        high = me.z + step

        @pl.when(low >= 0)
        def _():
            slot = jnp.maximum(low, 0)
            wait_for(kv.at[slot], sr.at[slot])

            @pl.when(me.z < 3)
            def _():
                kv_send(slot, 0).start()

        @pl.when(high <= 3)
        def _():
            slot = jnp.minimum(high, 3)
            wait_for(kv.at[slot], sr.at[slot])

            @pl.when(me.z > 0)
            def _():
                kv_send(slot, 1).start()

    gram = left_of(kv[0])
    for part in range(1, 4):
        gram += left_of(kv[part])
    out_kv[...] = update_of(gram, kv[me.z])

    for k in range(5):
        q, slot = slot_of(5 * me.owner + k)
        src = g_ref.at[:, k * UNIT : (k + 1) * UNIT]
        for zh in range(2):
            @pl.when(jnp.logical_not(jnp.logical_and(q == me.z, me.zh == zh)))
            def _():
                wait_for(src, gs1.at[k, zh])

    for step, x in quarters:
        for k in range(5):
            q, src, dst, group = quarter_unit(x, step, k)

            @pl.when(q != me.z)
            def _():
                wait_for(src, p1s.at[step, k])

    @pl.loop(0, 4)
    def _(group):
        p_sent(group)

    @pl.loop(0, 5)
    def _(k):
        g_origin(k, True)
        g_next(k, True)
        g_last(k, True)

    for copy in own_q + sum_q:
        copy.wait_recv()
    square = (qw + ql[...].astype(F32) + qr[...].astype(F32)).astype(BF16)
    out_q[...] = update_of(left_of(square), square)

    c_far.wait_recv()
    out_c[...] = (
        cp[me.z].astype(F32) + ca[me.z // 2].astype(F32) + cb[1].astype(F32)
    ).astype(BF16)

    for origin in range(4):
        block = xg.at[origin * tokens : (origin + 1) * tokens]

        @pl.when(jnp.logical_and(origin <= me.z, me.z < 3))
        def _():
            wait_for(block, xs.at[0, origin])
            wait_for(kv.at[origin], ss.at[0, origin])

        @pl.when(jnp.logical_and(origin >= me.z, me.z > 0))
        def _():
            wait_for(block, xs.at[1, origin])
            wait_for(kv.at[origin], ss.at[1, origin])

    for copy in raw_k + own_k + sum_k + raw_q + own_q + sum_q + c_near + [c_far] + scatter:
        copy.wait_send()


def dma(*shape):
    return pltpu.SemaphoreType.DMA(shape)


def split(value):
    high = value.astype(BF16)
    return high, (value - high.astype(F32)).astype(BF16)


def mm(a, b):
    return lax.dot_general(a, b, (((1,), (0,)), ((), ())), preferred_element_type=F32)


def update_of(left, target):
    width = left.shape[0]
    scale = math.sqrt(width) * jnp.sqrt(jnp.mean(left * left) + 1e-06)
    lh, ll = split(left * (1.0 / scale))
    once = mm(lh, target) + mm(ll, target)
    oh, ol = split(once)
    twice = mm(lh, oh) + mm(ll, oh) + mm(lh, ol)
    factor = math.sqrt(width) / 16.0 * lax.rsqrt(scale)
    return (factor * (25.0 * target.astype(F32) - 10.0 * once + twice)).astype(BF16)


def left_of(block):
    return lax.dot_general(block, block, (((1,), (1,)), ((), ())), preferred_element_type=F32)


def body(layer_input, output_grads, projection):
    tokens, rows = layer_input.shape
    half = rows // 2
    shape = jax.ShapeDtypeStruct
    vmem = pl.BlockSpec(memory_space=pltpu.VMEM)

    def space(*dims):
        return pltpu.VMEM(dims, BF16)

    update_kv, grad_input, update_query, _ = pl.pallas_call(
        fused_kernel,
        name="fused",
        out_shape=(
            shape((rows, UNIT), BF16),
            shape((tokens, rows), BF16),
            shape((rows, BLOCK), BF16),
            shape((4, rows // 4, projection.shape[1]), BF16),
        ),
        in_specs=[pl.BlockSpec(memory_space=pl.ANY)] * 3,
        out_specs=(vmem, vmem, vmem, pl.BlockSpec(memory_space=pl.ANY)),
        scratch_shapes=[
            space(4 * tokens, rows),
            space(rows, 4 * tokens),
            space(4 * tokens, SLOTS * UNIT),
            space(rows, SLOTS * UNIT),
            space(3, rows, UNIT),
            space(3, rows, BLOCK),
            space(2, half, UNIT),
            space(2, half, BLOCK),
            space(rows, UNIT),
            space(rows, UNIT),
            space(rows, BLOCK),
            space(rows, BLOCK),
            space(4, rows, UNIT),
            space(4, tokens, rows),
            space(2, tokens, rows),
            space(2, tokens, rows),
            dma(5, 2),
            dma(SLOTS, 3),
            dma(SLOTS, 4),
            dma(4),
            dma(4),
            dma(4, 5),
            dma(4),
            dma(2, 4),
            dma(2, 4),
            dma(4, 4),
            dma(4),
            dma(2, 4),
            dma(4),
            dma(2),
            dma(2),
            dma(2),
            dma(2),
            dma(4),
            dma(4),
            dma(4),
            dma(4),
            dma(2, 4),
            dma(4),
            dma(3),
            dma(3),
        ],
        compiler_params=pltpu.CompilerParams(
            collective_id=0, has_side_effects=True, vmem_limit_bytes=VMEM_LIMIT
        ),
    )(layer_input, output_grads, projection)
    return (grad_input, update_query, update_kv)


def solution(mesh):
    placed = (P("dp", "owner"), P("dp", "owner"), P("owner", "dp"))
    return jax.shard_map(
        body,
        mesh=mesh,
        in_specs=placed,
        out_specs=(P("dp", "owner"), P("owner", "dp"), P("owner", "dp")),
        check_vma=False,
    )
```
